32 devices in a mesh: pp: 4 (over x, core), tp: 4 (over z), dp: 2 (over y).
Axes of the slice: x: 2, y: 2, z: 4, core: 2. Of those that a mesh axis runs over, the one named last changes fastest.
Arguments:
- act_in: bfloat16 [4, 2, 128, 4096], P('pp', 'dp', 'tp'), may hold values from -6 to 6
- stash_in: bfloat16 [4, 2, 128, 4096], P('pp', 'dp', 'tp'), may hold values from -6 to 6
- grad_in: bfloat16 [4, 2, 128, 4096], P('pp', 'dp', 'tp'), may hold values from -6 to 6
- doc_ids: int32 [4, 2, 2, 128], P('pp', 'dp'), may hold values from 0 to 15, never falling along the last dimension, each value on 1 to 64 neighbouring positions
- query_weight: bfloat16 [4, 4096, 4096], P('pp', None, 'tp'), as said below
- key_weight: bfloat16 [4, 4096, 1024], P('pp', None, 'tp'), as said below
- value_weight: bfloat16 [4, 4096, 1024], P('pp', None, 'tp'), as said below
- out_weight: bfloat16 [4, 4096, 4096], P('pp', None, 'tp'), may hold values from -0.09375 to 0.09375
Outputs:
- act_out: bfloat16 [4, 2, 128, 4096], P('pp', 'dp', 'tp')
- grad_out: bfloat16 [4, 2, 128, 4096], P('pp', 'dp', 'tp')
- grad_query: float32 [4, 4096, 4096], P('pp', 'dp', 'tp')
- grad_key: float32 [4, 4096, 1024], P('pp', 'dp', 'tp')
- grad_value: float32 [4, 4096, 1024], P('pp', 'dp', 'tp')
The draws below stay inside these ranges and needn't reach their ends.
Inputs may be any that keep to these rules, and one draw needn't show every extreme that they name: `doc_ids`: along each row of 128 positions the document numbers never fall. `query_weight`: entries of mean zero. `key_weight`: for each of the 8 key heads, its 1 stored copies (consecutive blocks of 128 columns) are equal; entries of mean zero. `value_weight`: for each of the 8 value heads, its 1 stored copies (consecutive blocks of 128 columns) are equal.
All inputs are finite; a program needn't handle non-finite values.
Results may differ from the reference program's by a relative error of at most 0.033.
Values may be sent and summed in bfloat16 or wider, within the bound.
A program may use at most 128 MiB of HBM per device.

```python
import math
import jax
import jax.numpy as jnp
import numpy as np
from jax import lax

D = 4096
HEADS = 32
KV = 8
HEAD = 128
SEQ = 128
SPREAD = 1
N_PP = 4
N_TP = 4
N_DP = 2


def shared_heads(key, salt):
    base = jax.random.normal(jax.random.fold_in(key, salt), (N_PP, D, KV, 1, HEAD), jnp.float32)
    base = jnp.clip(base, -5.0, 5.0) / math.sqrt(D)
    return jnp.broadcast_to(base, (N_PP, D, KV, SPREAD, HEAD)).reshape(N_PP, D, KV * SPREAD, HEAD)


def draw_key_weight(key, part):
    return shared_heads(key, 11).reshape(N_PP, D, KV * SPREAD * HEAD).astype(jnp.bfloat16)


def draw_value_weight(key, part):
    return shared_heads(key, 13).reshape(N_PP, D, KV * SPREAD * HEAD).astype(jnp.bfloat16)


def draw_query_weight(key, part):
    fresh = jax.random.normal(jax.random.fold_in(key, 12), (N_PP, D, HEADS * HEAD), jnp.float32)
    fresh = jnp.clip(fresh, -5.0, 5.0) / math.sqrt(D)
    return fresh.astype(jnp.bfloat16)


def block_levels(key, dims, cuts, least, top_value):
    loudness = 1.0
    for axis_at, shards_of in cuts:
        heights = jax.random.uniform(jax.random.fold_in(jax.random.fold_in(key, 6), axis_at), (shards_of,), jnp.float32, least / len(cuts), top_value / len(cuts))
        loudness = loudness * jnp.repeat(jnp.exp(heights), dims[axis_at] // shards_of).reshape((-1,) + (1,) * (len(dims) - 1 - axis_at))
    return loudness


def profile(count, total, reach, skew):
    weights = [(1 << 20) // math.isqrt(grade ** skew) + 1 for grade in range(2, count + 1)]
    spare, given = total - reach - (count - 1), [1] * (count - 1)
    while spare > 0:
        movable = [i for i in range(count - 1) if given[i] < reach]
        whole, left = sum([weights[i] for i in movable]), spare
        for i in movable:
            addition = min(reach - given[i], max(1, left * weights[i] // whole), spare)
            given[i] = given[i] + addition
            spare = spare - addition
    return np.array([reach] + given)


def ragged_sizes(own_key, count, total, limit, slope):
    if count == 2:
        one = jax.random.randint(own_key, (), max(1, total - limit), min(limit, total - 1) + 1)
        return jnp.stack([one, total - one])
    lengths = jnp.asarray(profile(count, total, limit, slope), jnp.int32)
    twos = (count - 1) // 2
    giver, sink = lengths[1:1 + 2 * twos:2], lengths[2:2 + 2 * twos:2]
    room = jnp.minimum(giver - 1, limit - sink)
    passed = jax.random.randint(jax.random.fold_in(own_key, 1), (twos,), 0, 1 << 20) % (room + 1)
    lengths = lengths.at[1:1 + 2 * twos:2].set(giver - passed).at[2:2 + 2 * twos:2].set(sink + passed)
    return lengths[jax.random.permutation(jax.random.fold_in(own_key, 2), count)]


def noise(key, shape, deviation, limit, split=(), held_as=jnp.bfloat16):
    result = deviation * jax.random.normal(key, shape, jnp.float32)
    if split:
        result = result * block_levels(key, shape, split, -0.22, 0.18)
    return jnp.clip(result, -limit, limit).astype(held_as)


def setup_inputs(seed: int = 0) -> dict:
    streams_of = jax.random.split(jax.random.key(seed), 9)
    return {
        "act_in": noise(streams_of[0], (N_PP, N_DP, SEQ, D), 1.0, 6.0, ((0, 4), (1, 2), (2, 4))),
        "stash_in": noise(streams_of[1], (N_PP, N_DP, SEQ, D), 1.0, 6.0, ((0, 4), (1, 2), (2, 4))),
        "grad_in": noise(streams_of[2], (N_PP, N_DP, SEQ, D), 1.0, 6.0, ((0, 4), (1, 2), (2, 4))),
        "doc_ids": jax.vmap(lambda own: jnp.searchsorted(jnp.cumsum(ragged_sizes(own, SEQ // 8, SEQ, SEQ // 2, 2)), jnp.arange(SEQ), side="right"))(jax.random.split(streams_of[3], N_PP * N_DP * 2)).reshape((N_PP, N_DP, 2, SEQ)).astype(jnp.int32),
        "query_weight": draw_query_weight(jax.random.fold_in(streams_of[8], 71), 0),
        "key_weight": draw_key_weight(jax.random.fold_in(streams_of[8], 71), 0),
        "value_weight": draw_value_weight(jax.random.fold_in(streams_of[8], 71), 0),
        "out_weight": noise(streams_of[7], (N_PP, D, HEADS * HEAD), (HEADS * HEAD) ** -0.5, 0.09375, ((0, 4), (2, 4))),
    }


epsilon = 1e-05

def norm_rows(token_rows):
    widened = token_rows.astype(jnp.float32)
    inverse = lax.rsqrt(lax.optimization_barrier(jnp.mean(widened * widened, axis=-1, keepdims=True)) + epsilon)
    return ((widened * inverse).astype(jnp.bfloat16), inverse)

def allowed(documents):
    length = documents.shape[0]
    position = jnp.arange(length, dtype=jnp.int32)
    return (position[None, :] <= position[:, None]) & (documents[:, None] == documents[None, :])

def project(normed, weight):
    return jnp.dot(normed, weight, preferred_element_type=jnp.float32).astype(jnp.bfloat16)

def contract_first(left_side, right_side):
    return lax.dot_general(left_side, right_side, (((0,), (0,)), ((), ())), preferred_element_type=jnp.float32)

def split_heads(queries, keys, values):
    length = queries.shape[0]
    key_count = KV * SPREAD
    group_size = HEADS // key_count
    query_heads = queries.astype(jnp.float32).reshape(length, key_count, group_size, HEAD)
    key_heads = keys.astype(jnp.float32).reshape(length, key_count, HEAD)
    value_heads = values.astype(jnp.float32).reshape(length, key_count, HEAD)
    return (query_heads, key_heads, value_heads)

def attend(queries, keys, values, allowed_pairs):
    length = queries.shape[0]
    query_heads, key_heads, value_heads = split_heads(queries, keys, values)
    scores = jnp.einsum('ihgd,jhd->hgij', query_heads, key_heads) * (1.0 / math.sqrt(HEAD))
    scores = jnp.where(allowed_pairs, scores, -jnp.inf)
    row_max = lax.optimization_barrier(jnp.max(scores, axis=-1, keepdims=True))
    weights = jnp.exp(scores - row_max)
    probs = (weights / lax.optimization_barrier(jnp.sum(weights, axis=-1, keepdims=True))).astype(jnp.bfloat16)
    mixed = jnp.einsum('hgij,jhd->ihgd', probs.astype(jnp.float32), value_heads)
    return (probs, mixed.astype(jnp.bfloat16).reshape(length, HEADS * HEAD))

def attend_back(dmixed, queries, keys, values, probs):
    length = queries.shape[0]
    query_heads, key_heads, value_heads = split_heads(queries, keys, values)
    dmixed_heads = dmixed.astype(jnp.float32).reshape(query_heads.shape)
    dprobs = jnp.einsum('ihgd,jhd->hgij', dmixed_heads, value_heads)
    weights = probs.astype(jnp.float32)
    inner = lax.optimization_barrier(jnp.sum(weights * dprobs, axis=-1, keepdims=True))
    dscores = (weights * (dprobs - inner) * (1.0 / math.sqrt(HEAD))).astype(jnp.bfloat16)
    dqueries = jnp.einsum('hgij,jhd->ihgd', dscores.astype(jnp.float32), key_heads)
    dkeys = jnp.einsum('hgij,ihgd->jhd', dscores.astype(jnp.float32), query_heads)
    dvalues = jnp.einsum('hgij,ihgd->jhd', weights, dmixed_heads)
    return (dqueries.astype(jnp.bfloat16).reshape(length, HEADS * HEAD), dkeys.reshape(length, KV * SPREAD * HEAD), dvalues.reshape(length, KV * SPREAD * HEAD))

def rounded(product):
    return lax.optimization_barrier(product.astype(jnp.bfloat16)).astype(jnp.float32)

def group_sum(pairs):
    total = None
    for left_side, weight in pairs:
        length = left_side.shape[0]
        width = left_side.shape[1] // N_TP
        term = jnp.einsum('snc,dnc->nsd', left_side.astype(jnp.float32).reshape(length, N_TP, width), weight.astype(jnp.float32).reshape(weight.shape[0], N_TP, width))
        total = term if total is None else total + term
    return lax.optimization_barrier(jnp.sum(rounded(total), axis=0))

def section(inputs):
    forward_in, backward_in, incoming, documents, w_query, w_key, w_value, w_out = inputs

    def copy_step(totals, item):
        forward_rows, backward_rows, grad_rows, copy_docs = item
        normed_ahead, unused_inverse = norm_rows(forward_rows)
        probs_ahead, mixed_ahead = attend(project(normed_ahead, w_query), project(normed_ahead, w_key), project(normed_ahead, w_value), allowed(copy_docs[0]))
        attended = group_sum([(mixed_ahead, w_out)])
        outgoing = (forward_rows.astype(jnp.float32) + attended).astype(jnp.bfloat16)
        normed_back, inverse_back = norm_rows(backward_rows)
        queries = project(normed_back, w_query)
        keys = project(normed_back, w_key)
        values = project(normed_back, w_value)
        probs_back, unused_mixed = attend(queries, keys, values, allowed(copy_docs[1]))
        dmixed = jnp.dot(grad_rows, w_out, preferred_element_type=jnp.float32).astype(jnp.bfloat16)
        dqueries, dkeys, dvalues = attend_back(dmixed, queries, keys, values, probs_back)
        dkeys = dkeys.astype(jnp.bfloat16)
        dvalues = dvalues.astype(jnp.bfloat16)
        dnormed = group_sum([(dqueries, w_query), (dkeys, w_key), (dvalues, w_value)])
        scaled = backward_rows.astype(jnp.float32) * inverse_back
        grad_back = grad_rows.astype(jnp.float32) + inverse_back * (dnormed - scaled * lax.optimization_barrier(jnp.mean(dnormed * scaled, axis=-1, keepdims=True)))
        new_totals = (totals[0] + rounded(contract_first(normed_back, dqueries)), totals[1] + rounded(contract_first(normed_back, dkeys)), totals[2] + rounded(contract_first(normed_back, dvalues)))
        return (new_totals, (outgoing, grad_back.astype(jnp.bfloat16)))
    zeros = (jnp.zeros((D, HEADS * HEAD), jnp.float32), jnp.zeros((D, KV * SPREAD * HEAD), jnp.float32), jnp.zeros((D, KV * SPREAD * HEAD), jnp.float32))
    totals, (outgoing, grad_back) = lax.scan(copy_step, zeros, (forward_in, backward_in, incoming, documents))
    return (outgoing, grad_back, totals[0], totals[1], totals[2])

def reference(act_in, stash_in, grad_in, doc_ids, query_weight, key_weight, value_weight, out_weight):
    outgoing, grad_back, grad_query, grad_key, grad_value = lax.map(section, (act_in, stash_in, grad_in, doc_ids, query_weight, key_weight, value_weight, out_weight))
    act_out = jnp.roll(outgoing, 1, axis=0)
    grad_out = jnp.roll(grad_back, -1, axis=0)
    return (act_out, grad_out, grad_query, grad_key, grad_value)
```

```python
import functools
import math

import jax
import jax.numpy as jnp
from jax import lax
from jax.experimental import pallas as pl
from jax.experimental.pallas import tpu as pltpu
from jax.sharding import PartitionSpec as P

HEAD = 128
epsilon = 1e-05
MESH = pl.DeviceIdType.MESH
VMEM_LIMIT = 62 * 1024 * 1024
bf16 = jnp.bfloat16
f32 = jnp.float32


def remote(source, target, send_sem, recv_sem, axis, device):
    return pltpu.make_async_remote_copy(
        src_ref=source,
        dst_ref=target,
        send_sem=send_sem,
        recv_sem=recv_sem,
        device_id={axis: device},
        device_id_type=MESH,
    )


def contract_last(left, right):
    return lax.dot_general(left, right, (((1,), (1,)), ((), ())), preferred_element_type=f32)


def contract_first(left, right):
    return lax.dot_general(left, right, (((0,), (0,)), ((), ())), preferred_element_type=f32)


def chunking(rows, width):
    return (2, 4) if rows * width >= 32 * 4096 else (1, 1)


def section_kernel(
    n, copies, stages, gather_parts, sum_parts,
    stash, grad, act, docs, wq, wk, wv, wo,
    act_out, grad_out, ncols, aq, ak, av,
    full, inv, vq, vk, vv, vo, q, k, v, dm, mixed, probs, dq, dk, dv,
    sums, slots, total, outgoing,
    wsem, ss, rs, ts, tr, dss, drs, hs, hr,
):
    me = lax.axis_index("tp")
    mine = lax.axis_index("dp")
    stage = lax.axis_index("pp")
    rows, width = act.shape
    seq = rows * n
    piece = width // copies
    kv_local = vk.shape[1] // HEAD
    group = vq.shape[1] // (kv_local * HEAD)
    scale = 1.0 / math.sqrt(HEAD)
    own = (stash, grad, act)

    loads = []
    for i, (hbm, vmem) in enumerate(((wq, vq), (wk, vk), (wv, vv), (wo, vo))):
        load = pltpu.make_async_copy(hbm, vmem, wsem.at[i])
        load.start()
        loads.append(load)

    barrier = pltpu.get_barrier_semaphore()

    @pl.when(me > 0)
    def _():
        pl.semaphore_signal(barrier, inc=1, device_id={"tp": me - 1}, device_id_type=MESH)

    @pl.when(me < n - 1)
    def _():
        pl.semaphore_signal(barrier, inc=1, device_id={"tp": me + 1}, device_id_type=MESH)

    for offset in range(1, copies):
        other = lax.rem(mine + offset, copies)
        pl.semaphore_signal(barrier, inc=1, device_id={"dp": other}, device_id_type=MESH)
    ahead, behind = lax.rem(stage + 1, stages), lax.rem(stage + stages - 1, stages)
    for other in (ahead, behind):
        pl.semaphore_signal(barrier, inc=1, device_id={"pp": other}, device_id_type=MESH)
    ends = jnp.where(me > 0, 1, 0) + jnp.where(me < n - 1, 1, 0)
    pl.semaphore_wait(barrier, ends + copies - 1 + 2)

    def at_rows(index):
        return pl.ds(pl.multiple_of(index * rows, rows), rows)

    def part(c, parts):
        return pl.ds(c * (width // parts), width // parts)

    def hop(a, side, step, c):
        toward = 1 if side == 0 else -1
        carried = me - toward * (step - 1)
        columns = part(c, gather_parts)
        target = full.at[a, at_rows(carried), columns]
        source = own[a].at[:, columns] if step == 1 else target
        return remote(
            source, target, ss.at[a, side, step - 1, c], rs.at[a, side, step - 1, c],
            "tp", me + toward,
        )

    def sends(side, step):
        if side == 0:
            return (me < n - 1) & (me - (step - 1) >= 0)
        return (me > 0) & (me + (step - 1) < n)

    def gets(side, step):
        return (me - step >= 0) if side == 0 else (me + step < n)

    def start(a):
        for c in range(gather_parts):
            for side in range(2):
                @pl.when(sends(side, 1))
                def _():
                    hop(a, side, 1, c).start()

    def arrive(a, step):
        for c in range(gather_parts):
            for side in range(2):
                toward = 1 if side == 0 else -1

                @pl.when(gets(side, step))
                def _():
                    landed = full.at[a, at_rows(me - toward * step), part(c, gather_parts)]
                    remote(
                        landed, landed,
                        ss.at[a, side, step - 1, c], rs.at[a, side, step - 1, c], "tp",
                        jnp.where(me == 0, 1, me - 1),
                    ).wait_recv()

                if step < n - 1:
                    @pl.when(sends(side, step + 1))
                    def _():
                        hop(a, side, step + 1, c).start()

    def square(a, which, index):
        wide = full[a, at_rows(index), :].astype(f32)
        inverse = lax.rsqrt(jnp.mean(wide * wide, axis=-1, keepdims=True) + epsilon)
        inv[which, at_rows(index), :] = jnp.broadcast_to(inverse, (rows, HEAD))

    def arrive_square(a, which, step):
        arrive(a, step)
        for side in range(2):
            @pl.when(gets(side, step))
            def _():
                square(a, which, me - step if side == 0 else me + step)

    def multiply(a, right, out, which):
        tile = min(256, right.shape[1])

        @pl.loop(0, right.shape[1] // tile)
        def _(t):
            columns = pl.ds(pl.multiple_of(t * tile, tile), tile)
            product = jnp.dot(full[a], right[:, columns], preferred_element_type=f32)
            if which is not None:
                product = product * inv[which, :, :1]
            out[:, columns] = product.astype(bf16)

    def allowed(which):
        numbers = jnp.broadcast_to(docs[which : which + 1, :].astype(f32), (seq, seq))
        i = lax.broadcasted_iota(jnp.int32, (seq, seq), 0)
        j = lax.broadcasted_iota(jnp.int32, (seq, seq), 1)
        return (j <= i) & (numbers == numbers.T)

    def stack(ref, g):
        first = g * group
        return jnp.concatenate(
            [ref[:, (first + h) * HEAD : (first + h + 1) * HEAD] for h in range(group)], axis=0
        )

    def head(ref, g):
        return ref[:, g * HEAD : (g + 1) * HEAD]

    def probabilities(which, g):
        scores = contract_last(stack(q, g), head(k, g)) * scale
        pairs = allowed(which)
        scores = jnp.where(jnp.concatenate([pairs] * group, axis=0), scores, -jnp.inf)
        weights = jnp.exp(scores - jnp.max(scores, axis=-1, keepdims=True))
        return (weights / jnp.sum(weights, axis=-1, keepdims=True)).astype(bf16)

    def attend_back(g):
        weights = probs[g]
        wide = weights.astype(f32)
        stacked = stack(dm, g)
        dprobs = contract_last(stacked, head(v, g))
        inner = jnp.sum(wide * dprobs, axis=-1, keepdims=True)
        dscores = (wide * (dprobs - inner) * scale).astype(bf16)
        dqueries = jnp.dot(dscores, head(k, g), preferred_element_type=f32)
        inverse = inv[0, :, :]
        for h in range(group):
            columns = slice((g * group + h) * HEAD, (g * group + h + 1) * HEAD)
            one = dqueries[h * seq : (h + 1) * seq]
            dq[:, columns] = one.astype(bf16)
            aq[mine, :, columns] = (one * inverse).astype(bf16)
        columns = slice(g * HEAD, (g + 1) * HEAD)
        dkeys = contract_first(dscores, stack(q, g))
        dk[:, columns] = dkeys.astype(bf16)
        ak[mine, :, columns] = (dkeys * inverse).astype(bf16)
        dvalues = contract_first(weights, stacked)
        dv[:, columns] = dvalues.astype(bf16)
        av[mine, :, columns] = (dvalues * inverse).astype(bf16)

    def copy(a, side, dest, c, first):
        toward = 1 if side == 0 else -1
        columns = part(c, sum_parts)
        target = slots.at[a, side, dest, :, columns]
        source = sums.at[a, at_rows(dest), columns] if first else target
        return remote(
            source, target, ts.at[a, side, dest, c], tr.at[a, side, dest, c], "tp", me + toward
        )

    def landed(a, side, dest, c):
        slot = slots.at[a, side, dest, :, part(c, sum_parts)]
        remote(
            slot, slot, ts.at[a, side, dest, c], tr.at[a, side, dest, c], "tp",
            jnp.where(me == 0, 1, me - 1),
        ).wait_recv()

    def roles(side, dest):
        if side == 0:
            return me == 0, (me > 0) & (me < dest)
        return me == n - 1, (me < n - 1) & (me > dest)

    def route(side, turn):
        return n - 1 - turn if side == 0 else turn

    def first_send(a, turn, c):
        for side in range(2):
            dest = route(side, turn)

            @pl.when(roles(side, dest)[0])
            def _():
                copy(a, side, dest, c, True).start()

    def pass_on(a, turn, c):
        columns = part(c, sum_parts)
        for side in range(2):
            dest = route(side, turn)

            @pl.when(roles(side, dest)[1])
            def _():
                landed(a, side, dest, c)
                slots[a, side, dest, :, columns] = (
                    slots[a, side, dest, :, columns].astype(f32)
                    + sums[a, at_rows(dest), columns].astype(f32)
                ).astype(bf16)
                copy(a, side, dest, c, False).start()

    def collect(a, c, base):
        columns = part(c, sum_parts)
        mine_sum = sums[a, at_rows(me), columns].astype(f32)
        total[:, columns] = mine_sum if base is None else mine_sum + base[:, columns].astype(f32)
        for side in range(2):
            @pl.when(me > 0 if side == 0 else me < n - 1)
            def _():
                landed(a, side, me, c)
                total[:, columns] += slots[a, side, me, :, columns].astype(f32)

    def spread(a, pairs):
        tile = min(256, width // sum_parts)
        for c in range(sum_parts):
            base = c * (width // sum_parts)

            @pl.loop(0, width // sum_parts // tile)
            def _(t):
                features = pl.ds(pl.multiple_of(base + t * tile, tile), tile)
                acc = None
                for left, right in pairs:
                    term = contract_last(left[...], right[features, :])
                    acc = term if acc is None else acc + term
                sums[a, :, features] = acc.astype(bf16)

            first_send(a, 0, c)
        for turn in range(1, n - 1):
            for c in range(sum_parts):
                first_send(a, turn, c)

    start(0)
    for a in range(3):
        full[a, at_rows(me), :] = own[a][...]
    square(0, 0, me)
    square(2, 1, me)
    for step in range(1, n):
        arrive_square(0, 0, step)
        if step == max(n - 2, 1):
            start(1)
    trades = []

    def trade(i, source, target):
        for offset in range(1, copies):
            other = lax.rem(mine + offset, copies)
            one = remote(
                source(other), target, dss.at[offset, i], drs.at[offset, i], "dp", other
            )
            one.start()
            trades.append(one)

    trade(
        0, lambda other: full.at[0, :, pl.ds(pl.multiple_of(other * piece, piece), piece)],
        ncols.at[mine],
    )
    ncols[mine] = full[0, :, pl.ds(pl.multiple_of(mine * piece, piece), piece)]
    for load in loads:
        load.wait()
    multiply(0, vq, q, 0)
    arrive(1, 1)
    multiply(0, vk, k, 0)
    multiply(0, vv, v, 0)
    for g in range(kv_local):
        probs[g] = probabilities(1, g)
    for step in range(2, n):
        arrive(1, step)
        if step == max(n - 2, 1):
            start(2)
    multiply(1, vo, dm, None)
    for g in range(kv_local):
        attend_back(g)
    for i, target in enumerate((aq, ak, av)):
        trade(i + 1, lambda other: target.at[mine], target.at[mine])
    arrive_square(2, 1, 1)
    spread(0, ((dq, vq), (dk, vk), (dv, vv)))
    for step in range(2, n):
        arrive_square(2, 1, step)

    multiply(2, vq, q, 1)
    multiply(2, vk, k, 1)
    multiply(2, vv, v, 1)
    for g in range(kv_local):
        heads = jnp.dot(
            probabilities(0, g), head(v, g), preferred_element_type=f32
        ).astype(bf16)
        for h in range(group):
            columns = slice((g * group + h) * HEAD, (g * group + h + 1) * HEAD)
            mixed[:, columns] = heads[h * seq : (h + 1) * seq]
    spread(1, ((mixed, vo),))

    handoffs = []
    for turn in range(n - 1):
        for c in range(sum_parts):
            pass_on(0, turn, c)
    for c in range(sum_parts):
        collect(0, c, None)
    inverse = inv[0, at_rows(me), :1]
    scaled = stash[...].astype(f32) * inverse
    centred = total[...] - scaled * jnp.mean(total[...] * scaled, axis=-1, keepdims=True)
    outgoing[0] = (grad[...].astype(f32) + inverse * centred).astype(bf16)
    for c in range(sum_parts):
        columns = part(c, sum_parts)
        handoff = remote(
            outgoing.at[0, :, columns], grad_out.at[:, columns], hs.at[0, c], hr.at[0, c],
            "pp", behind,
        )
        handoff.start()
        handoffs.append(handoff)

    for turn in range(n - 1):
        for c in range(sum_parts):
            pass_on(1, turn, c)
    for c in range(sum_parts):
        columns = part(c, sum_parts)
        collect(1, c, act)
        outgoing[1, :, columns] = total[:, columns].astype(bf16)
        handoff = remote(
            outgoing.at[1, :, columns], act_out.at[:, columns], hs.at[1, c], hr.at[1, c],
            "pp", ahead,
        )
        handoff.start()
        handoffs.append(handoff)

    for a in range(3):
        for step in range(1, n):
            for c in range(gather_parts):
                for side in range(2):
                    @pl.when(sends(side, step))
                    def _():
                        hop(a, side, step, c).wait_send()
    for a in range(2):
        for turn in range(n - 1):
            for c in range(sum_parts):
                for side in range(2):
                    dest = route(side, turn)
                    first, middle = roles(side, dest)

                    @pl.when(first | middle)
                    def _():
                        copy(a, side, dest, c, False).wait_send()
    for one in trades + handoffs:
        one.wait()


def section_call(n, copies, stages, stash, grad, act, docs, wq, wk, wv, wo):
    rows, width = act.shape
    seq = rows * n
    gather_parts, sum_parts = chunking(rows, width)
    vmem = pl.BlockSpec(memory_space=pltpu.VMEM)
    anywhere = pl.BlockSpec(memory_space=pl.ANY)
    heads = wk.shape[1] // HEAD
    group = wq.shape[1] // wk.shape[1]
    shapes = [(rows, width), (rows, width), (copies, seq, width // copies)]
    shapes += [(copies, seq, w.shape[1]) for w in (wq, wk, wv)]
    sem = pltpu.SemaphoreType.DMA
    flops = 2 * seq * width * (3 * wq.shape[1] + 3 * wk.shape[1] + 3 * wv.shape[1] + wo.shape[1])
    return pl.pallas_call(
        functools.partial(section_kernel, n, copies, stages, gather_parts, sum_parts),
        out_shape=[jax.ShapeDtypeStruct(shape, bf16) for shape in shapes],
        in_specs=[vmem] * 4 + [anywhere] * 4,
        out_specs=[vmem] * len(shapes),
        scratch_shapes=[
            pltpu.VMEM((3, seq, width), bf16),
            pltpu.VMEM((2, seq, HEAD), f32),
        ]
        + [pltpu.VMEM(w.shape, bf16) for w in (wq, wk, wv, wo)]
        + [pltpu.VMEM((seq, w.shape[1]), bf16) for w in (wq, wk, wv, wo, wo)]
        + [pltpu.VMEM((heads, group * seq, seq), bf16)]
        + [pltpu.VMEM((seq, w.shape[1]), bf16) for w in (wq, wk, wv)]
        + [
            pltpu.VMEM((2, seq, width), bf16),
            pltpu.VMEM((2, 2, n, rows, width), bf16),
            pltpu.VMEM((rows, width), f32),
            pltpu.VMEM((2, rows, width), bf16),
            sem((4,)),
            sem((3, 2, n, gather_parts)), sem((3, 2, n, gather_parts)),
            sem((2, 2, n, sum_parts)), sem((2, 2, n, sum_parts)),
            sem((copies, 4)), sem((copies, 4)),
            sem((2, sum_parts)), sem((2, sum_parts)),
        ],
        compiler_params=pltpu.CompilerParams(
            collective_id=0, has_side_effects=True, vmem_limit_bytes=VMEM_LIMIT
        ),
        cost_estimate=pl.CostEstimate(
            flops=flops, bytes_accessed=30_000_000, transcendentals=0
        ),
    )(stash, grad, act, docs, wq, wk, wv, wo)


def weights_kernel(ncols, aq, ak, av, gq, gk, gv):
    left = ncols[...].reshape(-1, ncols.shape[2])
    for right, out in ((aq, gq), (ak, gk), (av, gv)):
        out[...] = contract_first(left, right[...].reshape(-1, right.shape[2]))


def weights_call(ncols, aq, ak, av):
    copies, seq, piece = ncols.shape
    tile = min(256, piece)
    whole = [pl.BlockSpec(g.shape, lambda t: (0, 0, 0)) for g in (aq, ak, av)]
    outs = [jax.ShapeDtypeStruct((piece, g.shape[2]), f32) for g in (aq, ak, av)]
    return pl.pallas_call(
        weights_kernel,
        grid=(piece // tile,),
        out_shape=outs,
        in_specs=[pl.BlockSpec((copies, seq, tile), lambda t: (0, 0, t))] + whole,
        out_specs=[pl.BlockSpec((tile, o.shape[1]), lambda t: (t, 0)) for o in outs],
        compiler_params=pltpu.CompilerParams(vmem_limit_bytes=40 * 1024 * 1024),
        cost_estimate=pl.CostEstimate(
            flops=2 * copies * seq * piece * sum(o.shape[1] for o in outs),
            bytes_accessed=4 * piece * sum(o.shape[1] for o in outs),
            transcendentals=0,
        ),
    )(ncols, aq, ak, av)


def body(act_in, stash_in, grad_in, doc_ids, query_weight, key_weight, value_weight, out_weight):
    n, copies, stages = (lax.axis_size(axis) for axis in ("tp", "dp", "pp"))
    act_out, grad_out, ncols, aq, ak, av = section_call(
        n, copies, stages, stash_in[0, 0], grad_in[0, 0], act_in[0, 0], doc_ids[0, 0],
        query_weight[0], key_weight[0], value_weight[0], out_weight[0],
    )
    grads = (grad[None] for grad in weights_call(ncols, aq, ak, av))
    return (act_out[None, None], grad_out[None, None], *grads)


def solution(mesh):
    placed = (
        P("pp", "dp", "tp", None),
        P("pp", "dp", "tp", None),
        P("pp", "dp", "tp", None),
        P("pp", "dp", None, None),
        P("pp", None, "tp"),
        P("pp", None, "tp"),
        P("pp", None, "tp"),
        P("pp", None, "tp"),
    )
    return jax.shard_map(
        body,
        mesh=mesh,
        in_specs=placed,
        out_specs=(
            P("pp", "dp", "tp", None),
            P("pp", "dp", "tp", None),
            P("pp", "dp", "tp"),
            P("pp", "dp", "tp"),
            P("pp", "dp", "tp"),
        ),
        check_vma=False,
    )
```

```python
import functools
import math

import jax
import jax.numpy as jnp
from jax import lax
from jax.experimental import pallas as pl
from jax.experimental.pallas import tpu as pltpu
from jax.sharding import PartitionSpec as P

HEAD = 128
epsilon = 1e-05
MESH = pl.DeviceIdType.MESH
VMEM_LIMIT = 62 * 1024 * 1024
bf16 = jnp.bfloat16
f32 = jnp.float32


def remote(source, target, send_sem, recv_sem, axis, device):
    return pltpu.make_async_remote_copy(
        src_ref=source,
        dst_ref=target,
        send_sem=send_sem,
        recv_sem=recv_sem,
        device_id={axis: device},
        device_id_type=MESH,
    )


def contract_last(left, right):
    return lax.dot_general(left, right, (((1,), (1,)), ((), ())), preferred_element_type=f32)


def contract_first(left, right):
    return lax.dot_general(left, right, (((0,), (0,)), ((), ())), preferred_element_type=f32)


def chunking(rows, width):
    return (2, 4) if rows * width >= 32 * 4096 else (1, 1)


def section_kernel(
    n, copies, stages, gather_parts, sum_parts,
    stash, grad, act, docs, wq, wk, wv, wo,
    act_out, grad_out, ncols, aq, ak, av,
    full, inv, vq, vk, vv, vo, q, k, v, dm, mixed, probs, dq, dk, dv,
    sums, slots, total, outgoing,
    wsem, ss, rs, ts, tr, dss, drs, hs, hr,
):
    me = lax.axis_index("tp")
    mine = lax.axis_index("dp")
    stage = lax.axis_index("pp")
    rows, width = act.shape
    seq = rows * n
    piece = width // copies
    kv_local = vk.shape[1] // HEAD
    group = vq.shape[1] // (kv_local * HEAD)
    scale = 1.0 / math.sqrt(HEAD)
    own = (stash, grad, act)

    loads = []
    for i, (hbm, vmem) in enumerate(((wq, vq), (wk, vk), (wv, vv), (wo, vo))):
        load = pltpu.make_async_copy(hbm, vmem, wsem.at[i])
        load.start()
        loads.append(load)

    barrier = pltpu.get_barrier_semaphore()

    @pl.when(me > 0)
    def _():
        pl.semaphore_signal(barrier, inc=1, device_id={"tp": me - 1}, device_id_type=MESH)

    @pl.when(me < n - 1)
    def _():
        pl.semaphore_signal(barrier, inc=1, device_id={"tp": me + 1}, device_id_type=MESH)

    for offset in range(1, copies):
        other = lax.rem(mine + offset, copies)
        pl.semaphore_signal(barrier, inc=1, device_id={"dp": other}, device_id_type=MESH)
    ahead, behind = lax.rem(stage + 1, stages), lax.rem(stage + stages - 1, stages)
    for other in (ahead, behind):
        pl.semaphore_signal(barrier, inc=1, device_id={"pp": other}, device_id_type=MESH)
    ends = jnp.where(me > 0, 1, 0) + jnp.where(me < n - 1, 1, 0)
    pl.semaphore_wait(barrier, ends + copies - 1 + 2)

    def at_rows(index):
        return pl.ds(pl.multiple_of(index * rows, rows), rows)

    def part(c, parts):
        return pl.ds(c * (width // parts), width // parts)

    def hop(a, side, step, c):
        toward = 1 if side == 0 else -1
        carried = me - toward * (step - 1)
        columns = part(c, gather_parts)
        target = full.at[a, at_rows(carried), columns]
        source = own[a].at[:, columns] if step == 1 else target
        return remote(
            source, target, ss.at[a, side, step - 1, c], rs.at[a, side, step - 1, c],
            "tp", me + toward,
        )

    def sends(side, step):
        if side == 0:
            return (me < n - 1) & (me - (step - 1) >= 0)
        return (me > 0) & (me + (step - 1) < n)

    def gets(side, step):
        return (me - step >= 0) if side == 0 else (me + step < n)

    def start(a):
        for c in range(gather_parts):
            for side in range(2):
                @pl.when(sends(side, 1))
                def _():
                    hop(a, side, 1, c).start()

    def arrive(a, step):
        for c in range(gather_parts):
            for side in range(2):
                toward = 1 if side == 0 else -1

                @pl.when(gets(side, step))
                def _():
                    landed = full.at[a, at_rows(me - toward * step), part(c, gather_parts)]
                    remote(
                        landed, landed,
                        ss.at[a, side, step - 1, c], rs.at[a, side, step - 1, c], "tp",
                        jnp.where(me == 0, 1, me - 1),
                    ).wait_recv()

                if step < n - 1:
                    @pl.when(sends(side, step + 1))
                    def _():
                        hop(a, side, step + 1, c).start()

    def square(a, which, index):
        wide = full[a, at_rows(index), :].astype(f32)
        inverse = lax.rsqrt(jnp.mean(wide * wide, axis=-1, keepdims=True) + epsilon)
        inv[which, at_rows(index), :] = jnp.broadcast_to(inverse, (rows, HEAD))

    def arrive_square(a, which, step):
        arrive(a, step)
        for side in range(2):
            @pl.when(gets(side, step))
            def _():
                square(a, which, me - step if side == 0 else me + step)

    def multiply(a, right, out, which):
        tile = min(256, right.shape[1])

        @pl.loop(0, right.shape[1] // tile)
        def _(t):
            columns = pl.ds(pl.multiple_of(t * tile, tile), tile)
            product = jnp.dot(full[a], right[:, columns], preferred_element_type=f32)
            if which is not None:
                product = product * inv[which, :, :1]
            out[:, columns] = product.astype(bf16)

    def allowed(which):
        numbers = jnp.broadcast_to(docs[which : which + 1, :].astype(f32), (seq, seq))
        i = lax.broadcasted_iota(jnp.int32, (seq, seq), 0)
        j = lax.broadcasted_iota(jnp.int32, (seq, seq), 1)
        return (j <= i) & (numbers == numbers.T)

    def stack(ref, g):
        first = g * group
        return jnp.concatenate(
            [ref[:, (first + h) * HEAD : (first + h + 1) * HEAD] for h in range(group)], axis=0
        )

    def head(ref, g):
        return ref[:, g * HEAD : (g + 1) * HEAD]

    def probabilities(which, g):
        scores = contract_last(stack(q, g), head(k, g)) * scale
        pairs = allowed(which)
        scores = jnp.where(jnp.concatenate([pairs] * group, axis=0), scores, -jnp.inf)
        weights = jnp.exp(scores - jnp.max(scores, axis=-1, keepdims=True))
        return (weights / jnp.sum(weights, axis=-1, keepdims=True)).astype(bf16)

    def attend_back(g):
        weights = probs[g]
        wide = weights.astype(f32)
        stacked = stack(dm, g)
        dprobs = contract_last(stacked, head(v, g))
        inner = jnp.sum(wide * dprobs, axis=-1, keepdims=True)
        dscores = (wide * (dprobs - inner) * scale).astype(bf16)
        dqueries = jnp.dot(dscores, head(k, g), preferred_element_type=f32)
        inverse = inv[0, :, :]
        for h in range(group):
            columns = slice((g * group + h) * HEAD, (g * group + h + 1) * HEAD)
            one = dqueries[h * seq : (h + 1) * seq]
            dq[:, columns] = one.astype(bf16)
            aq[mine, :, columns] = (one * inverse).astype(bf16)
        columns = slice(g * HEAD, (g + 1) * HEAD)
        dkeys = contract_first(dscores, stack(q, g))
        dk[:, columns] = dkeys.astype(bf16)
        ak[mine, :, columns] = (dkeys * inverse).astype(bf16)
        dvalues = contract_first(weights, stacked)
        dv[:, columns] = dvalues.astype(bf16)
        av[mine, :, columns] = (dvalues * inverse).astype(bf16)

    def copy(a, side, dest, c, first):
        toward = 1 if side == 0 else -1
        columns = part(c, sum_parts)
        target = slots.at[a, side, dest, :, columns]
        source = sums.at[a, at_rows(dest), columns] if first else target
        return remote(
            source, target, ts.at[a, side, dest, c], tr.at[a, side, dest, c], "tp", me + toward
        )

    def landed(a, side, dest, c):
        slot = slots.at[a, side, dest, :, part(c, sum_parts)]
        remote(
            slot, slot, ts.at[a, side, dest, c], tr.at[a, side, dest, c], "tp",
            jnp.where(me == 0, 1, me - 1),
        ).wait_recv()

    def roles(side, dest):
        if side == 0:
            return me == 0, (me > 0) & (me < dest)
        return me == n - 1, (me < n - 1) & (me > dest)

    def route(side, turn):
        return n - 1 - turn if side == 0 else turn

    def first_send(a, turn, c):
        for side in range(2):
            dest = route(side, turn)

            @pl.when(roles(side, dest)[0])
            def _():
                copy(a, side, dest, c, True).start()

    near = jnp.where(2 * me < n, 0, 1)

    def pass_on(a, turn):
        for side in (near, 1 - near):
            toward = 1 - 2 * side
            dest = jnp.where(side == 0, n - 1 - turn, turn)
            upward = (side == 0) & (me > 0) & (me < dest)
            downward = (side == 1) & (me < n - 1) & (me > dest)

            @pl.when(upward | downward)
            def _():
                for c in range(sum_parts):
                    columns = part(c, sum_parts)
                    landed(a, side, dest, c)
                    slots[a, side, dest, :, columns] = (
                        slots[a, side, dest, :, columns].astype(f32)
                        + sums[a, at_rows(dest), columns].astype(f32)
                    ).astype(bf16)
                    slot = slots.at[a, side, dest, :, columns]
                    remote(
                        slot, slot, ts.at[a, side, dest, c], tr.at[a, side, dest, c], "tp",
                        me + toward,
                    ).start()

    def collect(a, c, base):
        columns = part(c, sum_parts)
        mine_sum = sums[a, at_rows(me), columns].astype(f32)
        total[:, columns] = mine_sum if base is None else mine_sum + base[:, columns].astype(f32)
        for side in range(2):
            @pl.when(me > 0 if side == 0 else me < n - 1)
            def _():
                landed(a, side, me, c)
                total[:, columns] += slots[a, side, me, :, columns].astype(f32)

    def spread(a, pairs):
        tile = min(256, width // sum_parts)
        for c in range(sum_parts):
            base = c * (width // sum_parts)

            @pl.loop(0, width // sum_parts // tile)
            def _(t):
                features = pl.ds(pl.multiple_of(base + t * tile, tile), tile)
                acc = None
                for left, right in pairs:
                    term = contract_last(left[...], right[features, :])
                    acc = term if acc is None else acc + term
                sums[a, :, features] = acc.astype(bf16)

            first_send(a, 0, c)
        for turn in range(1, n - 1):
            for c in range(sum_parts):
                first_send(a, turn, c)

    start(0)
    for a in range(3):
        full[a, at_rows(me), :] = own[a][...]
    square(0, 0, me)
    square(2, 1, me)
    for step in range(1, n):
        arrive_square(0, 0, step)
        if step == max(n - 2, 1):
            start(1)
    trades = []

    def trade(i, source, target):
        for offset in range(1, copies):
            other = lax.rem(mine + offset, copies)
            one = remote(
                source(other), target, dss.at[offset, i], drs.at[offset, i], "dp", other
            )
            one.start()
            trades.append(one)

    trade(
        0, lambda other: full.at[0, :, pl.ds(pl.multiple_of(other * piece, piece), piece)],
        ncols.at[mine],
    )
    ncols[mine] = full[0, :, pl.ds(pl.multiple_of(mine * piece, piece), piece)]
    for load in loads:
        load.wait()
    multiply(0, vq, q, 0)
    arrive(1, 1)
    multiply(0, vk, k, 0)
    multiply(0, vv, v, 0)
    for g in range(kv_local):
        probs[g] = probabilities(1, g)
    for step in range(2, n):
        arrive(1, step)
        if step == max(n - 2, 1):
            start(2)
    multiply(1, vo, dm, None)
    for g in range(kv_local):
        attend_back(g)
    for i, target in enumerate((aq, ak, av)):
        trade(i + 1, lambda other: target.at[mine], target.at[mine])
    arrive_square(2, 1, 1)
    spread(0, ((dq, vq), (dk, vk), (dv, vv)))
    for step in range(2, n):
        arrive_square(2, 1, step)

    multiply(2, vq, q, 1)
    multiply(2, vk, k, 1)
    multiply(2, vv, v, 1)
    for g in range(kv_local):
        heads = jnp.dot(
            probabilities(0, g), head(v, g), preferred_element_type=f32
        ).astype(bf16)
        for h in range(group):
            columns = slice((g * group + h) * HEAD, (g * group + h + 1) * HEAD)
            mixed[:, columns] = heads[h * seq : (h + 1) * seq]
    spread(1, ((mixed, vo),))

    handoffs = []
    for turn in range(n - 1):
        pass_on(0, turn)
    for c in range(sum_parts):
        collect(0, c, None)
    inverse = inv[0, at_rows(me), :1]
    scaled = stash[...].astype(f32) * inverse
    centred = total[...] - scaled * jnp.mean(total[...] * scaled, axis=-1, keepdims=True)
    outgoing[0] = (grad[...].astype(f32) + inverse * centred).astype(bf16)
    for c in range(sum_parts):
        columns = part(c, sum_parts)
        handoff = remote(
            outgoing.at[0, :, columns], grad_out.at[:, columns], hs.at[0, c], hr.at[0, c],
            "pp", behind,
        )
        handoff.start()
        handoffs.append(handoff)

    for turn in range(n - 1):
        pass_on(1, turn)
    for c in range(sum_parts):
        columns = part(c, sum_parts)
        collect(1, c, act)
        outgoing[1, :, columns] = total[:, columns].astype(bf16)
        handoff = remote(
            outgoing.at[1, :, columns], act_out.at[:, columns], hs.at[1, c], hr.at[1, c],
            "pp", ahead,
        )
        handoff.start()
        handoffs.append(handoff)

    for a in range(3):
        for step in range(1, n):
            for c in range(gather_parts):
                for side in range(2):
                    @pl.when(sends(side, step))
                    def _():
                        hop(a, side, step, c).wait_send()
    for a in range(2):
        for turn in range(n - 1):
            for c in range(sum_parts):
                for side in range(2):
                    dest = route(side, turn)
                    first, middle = roles(side, dest)

                    @pl.when(first | middle)
                    def _():
                        copy(a, side, dest, c, False).wait_send()
    for one in trades + handoffs:
        one.wait()


def section_call(n, copies, stages, stash, grad, act, docs, wq, wk, wv, wo):
    rows, width = act.shape
    seq = rows * n
    gather_parts, sum_parts = chunking(rows, width)
    vmem = pl.BlockSpec(memory_space=pltpu.VMEM)
    anywhere = pl.BlockSpec(memory_space=pl.ANY)
    heads = wk.shape[1] // HEAD
    group = wq.shape[1] // wk.shape[1]
    shapes = [(rows, width), (rows, width), (copies, seq, width // copies)]
    shapes += [(copies, seq, w.shape[1]) for w in (wq, wk, wv)]
    sem = pltpu.SemaphoreType.DMA
    flops = 2 * seq * width * (3 * wq.shape[1] + 3 * wk.shape[1] + 3 * wv.shape[1] + wo.shape[1])
    return pl.pallas_call(
        functools.partial(section_kernel, n, copies, stages, gather_parts, sum_parts),
        out_shape=[jax.ShapeDtypeStruct(shape, bf16) for shape in shapes],
        in_specs=[vmem] * 4 + [anywhere] * 4,
        out_specs=[vmem] * len(shapes),
        scratch_shapes=[
            pltpu.VMEM((3, seq, width), bf16),
            pltpu.VMEM((2, seq, HEAD), f32),
        ]
        + [pltpu.VMEM(w.shape, bf16) for w in (wq, wk, wv, wo)]
        + [pltpu.VMEM((seq, w.shape[1]), bf16) for w in (wq, wk, wv, wo, wo)]
        + [pltpu.VMEM((heads, group * seq, seq), bf16)]
        + [pltpu.VMEM((seq, w.shape[1]), bf16) for w in (wq, wk, wv)]
        + [
            pltpu.VMEM((2, seq, width), bf16),
            pltpu.VMEM((2, 2, n, rows, width), bf16),
            pltpu.VMEM((rows, width), f32),
            pltpu.VMEM((2, rows, width), bf16),
            sem((4,)),
            sem((3, 2, n, gather_parts)), sem((3, 2, n, gather_parts)),
            sem((2, 2, n, sum_parts)), sem((2, 2, n, sum_parts)),
            sem((copies, 4)), sem((copies, 4)),
            sem((2, sum_parts)), sem((2, sum_parts)),
        ],
        compiler_params=pltpu.CompilerParams(
            collective_id=0, has_side_effects=True, vmem_limit_bytes=VMEM_LIMIT
        ),
        cost_estimate=pl.CostEstimate(
            flops=flops, bytes_accessed=30_000_000, transcendentals=0
        ),
    )(stash, grad, act, docs, wq, wk, wv, wo)


def weights_kernel(ncols, aq, ak, av, act_sent, grad_sent, gq, gk, gv, act_out, grad_out):
    left = ncols[...].reshape(-1, ncols.shape[2])
    for right, out in ((aq, gq), (ak, gk), (av, gv)):
        out[...] = contract_first(left, right[...].reshape(-1, right.shape[2]))
    act_out[...] = act_sent[...]
    grad_out[...] = grad_sent[...]


def weights_call(ncols, aq, ak, av, act_sent, grad_sent):
    copies, seq, piece = ncols.shape
    rows, width = act_sent.shape
    steps = max(1, piece // 256)
    tile = piece // steps
    whole = [pl.BlockSpec(g.shape, lambda t: (0, 0, 0)) for g in (aq, ak, av)]
    sent = [pl.BlockSpec((rows, width // steps), lambda t: (0, t))] * 2
    outs = [jax.ShapeDtypeStruct((piece, g.shape[2]), f32) for g in (aq, ak, av)]
    return pl.pallas_call(
        weights_kernel,
        grid=(steps,),
        out_shape=outs + [jax.ShapeDtypeStruct((rows, width), bf16)] * 2,
        in_specs=[pl.BlockSpec((copies, seq, tile), lambda t: (0, 0, t))] + whole + sent,
        out_specs=[pl.BlockSpec((tile, o.shape[1]), lambda t: (t, 0)) for o in outs] + sent,
        compiler_params=pltpu.CompilerParams(vmem_limit_bytes=VMEM_LIMIT),
        cost_estimate=pl.CostEstimate(
            flops=2 * copies * seq * piece * sum(o.shape[1] for o in outs),
            bytes_accessed=4 * piece * sum(o.shape[1] for o in outs),
            transcendentals=0,
        ),
    )(ncols, aq, ak, av, act_sent, grad_sent)


def body(act_in, stash_in, grad_in, doc_ids, query_weight, key_weight, value_weight, out_weight):
    n, copies, stages = (lax.axis_size(axis) for axis in ("tp", "dp", "pp"))
    act_sent, grad_sent, ncols, aq, ak, av = section_call(
        n, copies, stages, stash_in[0, 0], grad_in[0, 0], act_in[0, 0], doc_ids[0, 0],
        query_weight[0], key_weight[0], value_weight[0], out_weight[0],
    )
    grad_query, grad_key, grad_value, act_out, grad_out = weights_call(
        ncols, aq, ak, av, act_sent, grad_sent
    )
    return (
        act_out[None, None], grad_out[None, None],
        grad_query[None], grad_key[None], grad_value[None],
    )


def solution(mesh):
    placed = (
        P("pp", "dp", "tp", None),
        P("pp", "dp", "tp", None),
        P("pp", "dp", "tp", None),
        P("pp", "dp", None, None),
        P("pp", None, "tp"),
        P("pp", None, "tp"),
        P("pp", None, "tp"),
        P("pp", None, "tp"),
    )
    return jax.shard_map(
        body,
        mesh=mesh,
        in_specs=placed,
        out_specs=(
            P("pp", "dp", "tp", None),
            P("pp", "dp", "tp", None),
            P("pp", "dp", "tp"),
            P("pp", "dp", "tp"),
            P("pp", "dp", "tp"),
        ),
        check_vma=False,
    )
```

```python
import functools
import math

import jax
import jax.numpy as jnp
from jax import lax
from jax.experimental import pallas as pl
from jax.experimental.pallas import tpu as pltpu
from jax.sharding import PartitionSpec as P

HEAD = 128
epsilon = 1e-05
MESH = pl.DeviceIdType.MESH
VMEM_LIMIT = 40 * 1024 * 1024
bf16 = jnp.bfloat16
f32 = jnp.float32


def remote(source, target, send_sem, recv_sem, axis, device):
    return pltpu.make_async_remote_copy(
        src_ref=source,
        dst_ref=target,
        send_sem=send_sem,
        recv_sem=recv_sem,
        device_id={axis: device},
        device_id_type=MESH,
    )


def contract_last(left, right):
    return lax.dot_general(left, right, (((1,), (1,)), ((), ())), preferred_element_type=f32)


def contract_first(left, right):
    return lax.dot_general(left, right, (((0,), (0,)), ((), ())), preferred_element_type=f32)


def chunking(rows, width):
    return (4, 4) if rows * width >= 32 * 4096 else (1, 1)


def section_kernel(
    n, copies, stages, gather_parts, sum_parts,
    stash, grad, act, docs, wq, wk, wv, wo,
    act_out, grad_out, wgq, wgk, wgv,
    full, inv, vq, vk, vv, vo, q, k, v, dm, mixed, probs, dq, dk, dv,
    ncols, aq, ak, av, acc, sums, slots, total, outgoing,
    wsem, ss, rs, ts, tr, dss, drs, hs, hr,
):
    me = lax.axis_index("tp")
    mine = lax.axis_index("dp")
    stage = lax.axis_index("pp")
    rows, width = act.shape
    seq = rows * n
    piece = width // copies
    kv_local = vk.shape[1] // HEAD
    group = vq.shape[1] // (kv_local * HEAD)
    scale = 1.0 / math.sqrt(HEAD)

    def at_rows(index):
        return pl.ds(pl.multiple_of(index * rows, rows), rows)

    loads = []
    pairs = [(own, full.at[a, at_rows(me), :]) for a, own in enumerate((stash, grad, act))]
    pairs += [(wq, vq), (wk, vk), (wv, vv), (wo, vo)]
    for i, (hbm, vmem) in enumerate(pairs):
        load = pltpu.make_async_copy(hbm, vmem, wsem.at[i])
        load.start()
        loads.append(load)

    barrier = pltpu.get_barrier_semaphore()

    @pl.when(me > 0)
    def _():
        pl.semaphore_signal(barrier, inc=1, device_id={"tp": me - 1}, device_id_type=MESH)

    @pl.when(me < n - 1)
    def _():
        pl.semaphore_signal(barrier, inc=1, device_id={"tp": me + 1}, device_id_type=MESH)

    for offset in range(1, copies):
        other = lax.rem(mine + offset, copies)
        pl.semaphore_signal(barrier, inc=1, device_id={"dp": other}, device_id_type=MESH)
    ahead, behind = lax.rem(stage + 1, stages), lax.rem(stage + stages - 1, stages)
    for other in (ahead, behind):
        pl.semaphore_signal(barrier, inc=1, device_id={"pp": other}, device_id_type=MESH)
    ends = jnp.where(me > 0, 1, 0) + jnp.where(me < n - 1, 1, 0)
    pl.semaphore_wait(barrier, ends + copies - 1 + 2)

    def part(c, parts):
        return pl.ds(c * (width // parts), width // parts)

    def hop(a, side, step, c):
        toward = 1 if side == 0 else -1
        carried = me - toward * (step - 1)
        columns = part(c, gather_parts)
        block = full.at[a, at_rows(carried), columns]
        return remote(
            block, block, ss.at[a, side, step - 1, c], rs.at[a, side, step - 1, c],
            "tp", me + toward,
        )

    def sends(side, step):
        if side == 0:
            return (me < n - 1) & (me - (step - 1) >= 0)
        return (me > 0) & (me + (step - 1) < n)

    def gets(side, step):
        return (me - step >= 0) if side == 0 else (me + step < n)

    def start(a):
        for c in range(gather_parts):
            for side in range(2):
                @pl.when(sends(side, 1))
                def _():
                    hop(a, side, 1, c).start()

    def arrive(a, step, parts=None):
        for c in range(gather_parts) if parts is None else parts:
            for side in range(2):
                toward = 1 if side == 0 else -1

                @pl.when(gets(side, step))
                def _():
                    landed = full.at[a, at_rows(me - toward * step), part(c, gather_parts)]
                    remote(
                        landed, landed,
                        ss.at[a, side, step - 1, c], rs.at[a, side, step - 1, c], "tp",
                        jnp.where(me == 0, 1, me - 1),
                    ).wait_recv()

                if step < n - 1:
                    @pl.when(sends(side, step + 1))
                    def _():
                        hop(a, side, step + 1, c).start()

    def square(a, which, index):
        wide = full[a, at_rows(index), :].astype(f32)
        inverse = lax.rsqrt(jnp.mean(wide * wide, axis=-1, keepdims=True) + epsilon)
        inv[which, at_rows(index), :] = jnp.broadcast_to(inverse, (rows, HEAD))

    def squares(a, which, step):
        for side in range(2):
            @pl.when(gets(side, step))
            def _():
                square(a, which, me - step if side == 0 else me + step)

    def multiply(a, right, out, which, c=None, kept=0):
        tile = min(256, right.shape[1])
        features = slice(None) if c is None else part(c, gather_parts)

        @pl.loop(0, right.shape[1] // tile)
        def _(t):
            columns = pl.ds(pl.multiple_of(t * tile, tile), tile)
            held = pl.ds(pl.multiple_of(kept + t * tile, tile), tile)
            product = jnp.dot(
                full[a, :, features], right[features, columns], preferred_element_type=f32
            )
            if c is not None and c > 0:
                product = product + acc[:, held]
            if c is None or c == gather_parts - 1:
                if which is not None:
                    product = product * inv[which, :, :1]
                out[:, columns] = product.astype(bf16)
            else:
                acc[:, held] = product

    def allowed(which):
        numbers = jnp.broadcast_to(docs[which : which + 1, :].astype(f32), (seq, seq))
        i = lax.broadcasted_iota(jnp.int32, (seq, seq), 0)
        j = lax.broadcasted_iota(jnp.int32, (seq, seq), 1)
        return (j <= i) & (numbers == numbers.T)

    def stack(ref, g):
        first = g * group
        return jnp.concatenate(
            [ref[:, (first + h) * HEAD : (first + h + 1) * HEAD] for h in range(group)], axis=0
        )

    def head(ref, g):
        return ref[:, g * HEAD : (g + 1) * HEAD]

    def probabilities(which, g):
        scores = contract_last(stack(q, g), head(k, g)) * scale
        pairs = allowed(which)
        scores = jnp.where(jnp.concatenate([pairs] * group, axis=0), scores, -jnp.inf)
        weights = jnp.exp(scores - jnp.max(scores, axis=-1, keepdims=True))
        return (weights / jnp.sum(weights, axis=-1, keepdims=True)).astype(bf16)

    def attend_back(g):
        weights = probs[g]
        wide = weights.astype(f32)
        stacked = stack(dm, g)
        dprobs = contract_last(stacked, head(v, g))
        inner = jnp.sum(wide * dprobs, axis=-1, keepdims=True)
        dscores = (wide * (dprobs - inner) * scale).astype(bf16)
        dqueries = jnp.dot(dscores, head(k, g), preferred_element_type=f32)
        inverse = inv[0, :, :]
        for h in range(group):
            columns = slice((g * group + h) * HEAD, (g * group + h + 1) * HEAD)
            one = dqueries[h * seq : (h + 1) * seq]
            dq[:, columns] = one.astype(bf16)
            aq[mine, :, columns] = (one * inverse).astype(bf16)
        columns = slice(g * HEAD, (g + 1) * HEAD)
        dkeys = contract_first(dscores, stack(q, g))
        dk[:, columns] = dkeys.astype(bf16)
        ak[mine, :, columns] = (dkeys * inverse).astype(bf16)
        dvalues = contract_first(weights, stacked)
        dv[:, columns] = dvalues.astype(bf16)
        av[mine, :, columns] = (dvalues * inverse).astype(bf16)

    def copy(a, side, dest, c, first):
        toward = 1 if side == 0 else -1
        columns = part(c, sum_parts)
        target = slots.at[a, side, dest, :, columns]
        source = sums.at[a, at_rows(dest), columns] if first else target
        return remote(
            source, target, ts.at[a, side, dest, c], tr.at[a, side, dest, c], "tp", me + toward
        )

    def landed(a, side, dest, c):
        slot = slots.at[a, side, dest, :, part(c, sum_parts)]
        remote(
            slot, slot, ts.at[a, side, dest, c], tr.at[a, side, dest, c], "tp",
            jnp.where(me == 0, 1, me - 1),
        ).wait_recv()

    def roles(side, dest):
        if side == 0:
            return me == 0, (me > 0) & (me < dest)
        return me == n - 1, (me < n - 1) & (me > dest)

    def route(side, turn):
        return n - 1 - turn if side == 0 else turn

    def first_send(a, turn, c):
        for side in range(2):
            dest = route(side, turn)

            @pl.when(roles(side, dest)[0])
            def _():
                copy(a, side, dest, c, True).start()

    near = jnp.where(2 * me < n, 0, 1)

    def pass_on(a, turn, side):
        toward = 1 - 2 * side
        dest = jnp.where(side == 0, n - 1 - turn, turn)
        upward = (side == 0) & (me > 0) & (me < dest)
        downward = (side == 1) & (me < n - 1) & (me > dest)

        @pl.when(upward | downward)
        def _():
            for c in range(sum_parts):
                columns = part(c, sum_parts)
                landed(a, side, dest, c)
                slots[a, side, dest, :, columns] = (
                    slots[a, side, dest, :, columns].astype(f32)
                    + sums[a, at_rows(dest), columns].astype(f32)
                ).astype(bf16)
                slot = slots.at[a, side, dest, :, columns]
                remote(
                    slot, slot, ts.at[a, side, dest, c], tr.at[a, side, dest, c], "tp",
                    me + toward,
                ).start()

    def pass_all(a):
        for side in (near, 1 - near):
            for turn in range(n - 1):
                pass_on(a, turn, side)

    def collect(a, c, base):
        columns = part(c, sum_parts)
        mine_sum = sums[a, at_rows(me), columns].astype(f32)
        if base is not None:
            mine_sum = mine_sum + full[base, at_rows(me), columns].astype(f32)
        total[:, columns] = mine_sum
        for side in range(2):
            @pl.when(me > 0 if side == 0 else me < n - 1)
            def _():
                landed(a, side, me, c)
                total[:, columns] += slots[a, side, me, :, columns].astype(f32)

    def spread(a, pairs):
        tile = min(256, width // sum_parts)
        for c in range(sum_parts):
            base = c * (width // sum_parts)

            @pl.loop(0, width // sum_parts // tile)
            def _(t):
                features = pl.ds(pl.multiple_of(base + t * tile, tile), tile)
                acc = None
                for left, right in pairs:
                    term = contract_last(left[...], right[features, :])
                    acc = term if acc is None else acc + term
                sums[a, :, features] = acc.astype(bf16)

            first_send(a, 0, c)
        for turn in range(1, n - 1):
            for c in range(sum_parts):
                first_send(a, turn, c)

    loads[0].wait()
    start(0)
    square(0, 0, me)
    loads[1].wait()
    loads[2].wait()
    square(2, 1, me)
    for step in range(1, n):
        arrive(0, step)
        squares(0, 0, step)
        if step == max(n - 2, 1):
            start(1)
    trades = []

    def trade(i, source, target):
        for offset in range(1, copies):
            other = lax.rem(mine + offset, copies)
            one = remote(
                source(other), target, dss.at[offset, i], drs.at[offset, i], "dp", other
            )
            one.start()
            trades.append(one)

    trade(
        0, lambda other: full.at[0, :, pl.ds(pl.multiple_of(other * piece, piece), piece)],
        ncols.at[mine],
    )
    ncols[mine] = full[0, :, pl.ds(pl.multiple_of(mine * piece, piece), piece)]
    for load in loads[3:]:
        load.wait()
    multiply(0, vq, q, 0)
    arrive(1, 1)
    multiply(0, vk, k, 0)
    multiply(0, vv, v, 0)
    for g in range(kv_local):
        probs[g] = probabilities(1, g)
    for step in range(2, n - 1):
        arrive(1, step)
    start(2)
    for c in range(gather_parts):
        if n > 2:
            arrive(1, n - 1, (c,))
        multiply(1, vo, dm, None, c)
    for g in range(kv_local):
        attend_back(g)
    for i, target in enumerate((aq, ak, av)):
        trade(i + 1, lambda other: target.at[mine], target.at[mine])
    spread(0, ((dq, vq), (dk, vk), (dv, vv)))

    for step in range(1, n - 1):
        arrive(2, step)
        squares(2, 1, step)
    for c in range(gather_parts):
        arrive(2, n - 1, (c,))
        if c == gather_parts - 1:
            squares(2, 1, n - 1)
        kept = 0
        for right, out in ((vq, q), (vk, k), (vv, v)):
            multiply(2, right, out, 1, c, kept)
            kept += right.shape[1]
    for g in range(kv_local):
        heads = jnp.dot(
            probabilities(0, g), head(v, g), preferred_element_type=f32
        ).astype(bf16)
        for h in range(group):
            columns = slice((g * group + h) * HEAD, (g * group + h + 1) * HEAD)
            mixed[:, columns] = heads[h * seq : (h + 1) * seq]
    spread(1, ((mixed, vo),))

    pass_all(0)
    for one in trades:
        one.wait()
    tile = min(256, piece)

    @pl.loop(0, piece // tile)
    def _(t):
        features = pl.ds(pl.multiple_of(t * tile, tile), tile)
        left = ncols[:, :, features].reshape(copies * seq, tile)
        for right, out in ((aq, wgq), (ak, wgk), (av, wgv)):
            out[features, :] = contract_first(
                left, right[...].reshape(copies * seq, right.shape[2])
            )

    handoffs = []
    for c in range(sum_parts):
        collect(0, c, None)
    inverse = inv[0, at_rows(me), :1]
    scaled = full[0, at_rows(me), :].astype(f32) * inverse
    centred = total[...] - scaled * jnp.mean(total[...] * scaled, axis=-1, keepdims=True)
    outgoing[0] = (full[1, at_rows(me), :].astype(f32) + inverse * centred).astype(bf16)
    for c in range(sum_parts):
        columns = part(c, sum_parts)
        handoff = remote(
            outgoing.at[0, :, columns], grad_out.at[:, columns], hs.at[0, c], hr.at[0, c],
            "pp", behind,
        )
        handoff.start()
        handoffs.append(handoff)

    pass_all(1)
    for c in range(sum_parts):
        columns = part(c, sum_parts)
        collect(1, c, 2)
        outgoing[1, :, columns] = total[:, columns].astype(bf16)
        handoff = remote(
            outgoing.at[1, :, columns], act_out.at[:, columns], hs.at[1, c], hr.at[1, c],
            "pp", ahead,
        )
        handoff.start()
        handoffs.append(handoff)

    for a in range(3):
        for step in range(1, n):
            for c in range(gather_parts):
                for side in range(2):
                    @pl.when(sends(side, step))
                    def _():
                        hop(a, side, step, c).wait_send()
    for a in range(2):
        for turn in range(n - 1):
            for c in range(sum_parts):
                for side in range(2):
                    dest = route(side, turn)
                    first, middle = roles(side, dest)

                    @pl.when(first | middle)
                    def _():
                        copy(a, side, dest, c, False).wait_send()
    for one in handoffs:
        one.wait()


def pin(x):
    return pltpu.with_memory_space_constraint(x, pltpu.HBM)


def section_call(n, copies, stages, stash, grad, act, docs, wq, wk, wv, wo):
    rows, width = act.shape
    seq = rows * n
    gather_parts, sum_parts = chunking(rows, width)
    vmem = pl.BlockSpec(memory_space=pltpu.VMEM)
    hbm = pl.BlockSpec(memory_space=pltpu.HBM)
    heads = wk.shape[1] // HEAD
    group = wq.shape[1] // wk.shape[1]
    piece = width // copies
    outs = [jax.ShapeDtypeStruct((rows, width), bf16)] * 2
    outs += [jax.ShapeDtypeStruct((piece, w.shape[1]), f32) for w in (wq, wk, wv)]
    held = wq.shape[1] + wk.shape[1] + wv.shape[1]
    sem = pltpu.SemaphoreType.DMA
    flops = 2 * seq * width * (3 * wq.shape[1] + 3 * wk.shape[1] + 3 * wv.shape[1] + wo.shape[1])
    return pl.pallas_call(
        functools.partial(section_kernel, n, copies, stages, gather_parts, sum_parts),
        out_shape=outs,
        in_specs=[hbm] * 3 + [vmem] + [hbm] * 4,
        out_specs=[vmem] * len(outs),
        scratch_shapes=[
            pltpu.VMEM((3, seq, width), bf16),
            pltpu.VMEM((2, seq, HEAD), f32),
        ]
        + [pltpu.VMEM(w.shape, bf16) for w in (wq, wk, wv, wo)]
        + [pltpu.VMEM((seq, w.shape[1]), bf16) for w in (wq, wk, wv, wo, wo)]
        + [pltpu.VMEM((heads, group * seq, seq), bf16)]
        + [pltpu.VMEM((seq, w.shape[1]), bf16) for w in (wq, wk, wv)]
        + [pltpu.VMEM((copies, seq, piece), bf16)]
        + [pltpu.VMEM((copies, seq, w.shape[1]), bf16) for w in (wq, wk, wv)]
        + [
            pltpu.VMEM((seq, held), f32),
            pltpu.VMEM((2, seq, width), bf16),
            pltpu.VMEM((2, 2, n, rows, width), bf16),
            pltpu.VMEM((rows, width), f32),
            pltpu.VMEM((2, rows, width), bf16),
            sem((7,)),
            sem((3, 2, n, gather_parts)), sem((3, 2, n, gather_parts)),
            sem((2, 2, n, sum_parts)), sem((2, 2, n, sum_parts)),
            sem((copies, 4)), sem((copies, 4)),
            sem((2, sum_parts)), sem((2, sum_parts)),
        ],
        compiler_params=pltpu.CompilerParams(
            collective_id=0, has_side_effects=True, vmem_limit_bytes=VMEM_LIMIT
        ),
        cost_estimate=pl.CostEstimate(
            flops=flops, bytes_accessed=30_000_000, transcendentals=0
        ),
    )(*(pin(x) for x in (stash, grad, act)), docs, *(pin(x) for x in (wq, wk, wv, wo)))


def store_kernel(*refs):
    count = (len(refs) - 1) // 2
    sems = refs[-1]
    copies = []
    for i, (source, target) in enumerate(zip(refs[:count], refs[count:-1])):
        pieces = max(1, source.shape[0] // 512)
        size = source.shape[0] // pieces
        for p in range(pieces):
            where = pl.ds(p * size, size)
            one = pltpu.make_async_copy(source.at[where], target.at[where], sems.at[i, p])
            one.start()
            copies.append(one)
    for one in copies:
        one.wait()


def store_call(*arrays):
    pieces = max(1, max(a.shape[0] for a in arrays) // 512)
    return pl.pallas_call(
        store_kernel,
        out_shape=[jax.ShapeDtypeStruct(a.shape, a.dtype) for a in arrays],
        in_specs=[pl.BlockSpec(memory_space=pltpu.VMEM)] * len(arrays),
        out_specs=[pl.BlockSpec(memory_space=pltpu.HBM)] * len(arrays),
        scratch_shapes=[pltpu.SemaphoreType.DMA((len(arrays), pieces))],
        compiler_params=pltpu.CompilerParams(vmem_limit_bytes=20 * 1024 * 1024),
        cost_estimate=pl.CostEstimate(
            flops=10_000_000, bytes_accessed=sum(2 * a.size * a.dtype.itemsize for a in arrays),
            transcendentals=0,
        ),
    )(*arrays)


def body(act_in, stash_in, grad_in, doc_ids, query_weight, key_weight, value_weight, out_weight):
    n, copies, stages = (lax.axis_size(axis) for axis in ("tp", "dp", "pp"))
    made = section_call(
        n, copies, stages, stash_in[0, 0], grad_in[0, 0], act_in[0, 0], doc_ids[0, 0],
        query_weight[0], key_weight[0], value_weight[0], out_weight[0],
    )
    act_out, grad_out, grad_query, grad_key, grad_value = store_call(*made)
    return (
        act_out[None, None], grad_out[None, None],
        grad_query[None], grad_key[None], grad_value[None],
    )


def solution(mesh):
    placed = (
        P("pp", "dp", "tp", None),
        P("pp", "dp", "tp", None),
        P("pp", "dp", "tp", None),
        P("pp", "dp", None, None),
        P("pp", None, "tp"),
        P("pp", None, "tp"),
        P("pp", None, "tp"),
        P("pp", None, "tp"),
    )
    return jax.shard_map(
        body,
        mesh=mesh,
        in_specs=placed,
        out_specs=(
            P("pp", "dp", "tp", None),
            P("pp", "dp", "tp", None),
            P("pp", "dp", "tp"),
            P("pp", "dp", "tp"),
            P("pp", "dp", "tp"),
        ),
        check_vma=False,
    )
```

```python
import functools
import math

import jax
import jax.numpy as jnp
from jax import lax
from jax.experimental import pallas as pl
from jax.experimental.pallas import tpu as pltpu
from jax.sharding import PartitionSpec as P

HEAD = 128
epsilon = 1e-05
MESH = pl.DeviceIdType.MESH
VMEM_LIMIT = 40 * 1024 * 1024
bf16 = jnp.bfloat16
f32 = jnp.float32


def remote(source, target, send_sem, recv_sem, axis, device):
    return pltpu.make_async_remote_copy(
        src_ref=source,
        dst_ref=target,
        send_sem=send_sem,
        recv_sem=recv_sem,
        device_id={axis: device},
        device_id_type=MESH,
    )


def contract_last(left, right):
    return lax.dot_general(left, right, (((1,), (1,)), ((), ())), preferred_element_type=f32)


def contract_first(left, right):
    return lax.dot_general(left, right, (((0,), (0,)), ((), ())), preferred_element_type=f32)


def chunking(rows, width):
    if rows * width < 32 * 4096:
        return 1, ((width,), (width,))
    eighth = width // 8
    return 4, (
        tuple(eighth * k for k in (1, 1, 2, 2, 2)),
        tuple(eighth * k for k in (1, 2, 2, 1, 1, 1)),
    )


def section_kernel(
    n, copies, stages, gather_parts, cuts,
    stash, grad, act, numbers, wq, wk, wv, wo,
    act_out, grad_out, wgq, wgk, wgv,
    docs, full, inv, vq, vk, vv, vo, q, k, v, dm, mixed, probs, dq, dk, dv,
    ncols, aq, ak, av, acc, sums, slots, total, outgoing,
    wsem, ss, rs, ts, tr_back, tr_ahead, dss, drs, hs, hr,
):
    me = lax.axis_index("tp")
    mine = lax.axis_index("dp")
    stage = lax.axis_index("pp")
    rows, width = act.shape
    seq = rows * n
    piece = width // copies
    kv_local = vk.shape[1] // HEAD
    group = vq.shape[1] // (kv_local * HEAD)
    scale = 1.0 / math.sqrt(HEAD)

    def at_rows(index):
        return pl.ds(pl.multiple_of(index * rows, rows), rows)

    loads = []
    pairs = [(own, full.at[a, at_rows(me), :]) for a, own in enumerate((stash, grad, act))]
    pairs += [(wq, vq), (wk, vk), (wv, vv), (wo, vo), (numbers, docs)]
    for i, (hbm, vmem) in enumerate(pairs):
        load = pltpu.make_async_copy(hbm, vmem, wsem.at[i])
        load.start()
        loads.append(load)

    barrier = pltpu.get_barrier_semaphore()

    @pl.when(me > 0)
    def _():
        pl.semaphore_signal(barrier, inc=1, device_id={"tp": me - 1}, device_id_type=MESH)

    @pl.when(me < n - 1)
    def _():
        pl.semaphore_signal(barrier, inc=1, device_id={"tp": me + 1}, device_id_type=MESH)

    for offset in range(1, copies):
        other = lax.rem(mine + offset, copies)
        pl.semaphore_signal(barrier, inc=1, device_id={"dp": other}, device_id_type=MESH)
    ahead, behind = lax.rem(stage + 1, stages), lax.rem(stage + stages - 1, stages)
    for other in (ahead, behind):
        pl.semaphore_signal(barrier, inc=1, device_id={"pp": other}, device_id_type=MESH)
    ends = jnp.where(me > 0, 1, 0) + jnp.where(me < n - 1, 1, 0)
    pl.semaphore_wait(barrier, ends + copies - 1 + 2)

    def part(c):
        return pl.ds(c * (width // gather_parts), width // gather_parts)

    def cut(a, c):
        return pl.ds(sum(cuts[a][:c]), cuts[a][c])

    every = pl.ds(0, width)
    tr = (tr_back, tr_ahead)

    def hop(a, side, step, columns):
        toward = 1 if side == 0 else -1
        carried = me - toward * (step - 1)
        block = full.at[a, at_rows(carried), columns]
        return remote(
            block, block, ss.at[a, side, step - 1],
            rs.at[a, side, step - 1, columns.start * gather_parts // width],
            "tp", me + toward,
        )

    def sends(side, step):
        if side == 0:
            return (me < n - 1) & (me - (step - 1) >= 0)
        return (me > 0) & (me + (step - 1) < n)

    def gets(side, step):
        return (me - step >= 0) if side == 0 else (me + step < n)

    def start(a):
        for c in range(gather_parts):
            for side in range(2):
                @pl.when(sends(side, 1))
                def _():
                    hop(a, side, 1, part(c)).start()

    def arrive(a, step, parts=None):
        for c in range(gather_parts) if parts is None else parts:
            for side in range(2):
                toward = 1 if side == 0 else -1

                @pl.when(gets(side, step))
                def _():
                    landed = full.at[a, at_rows(me - toward * step), part(c)]
                    remote(
                        landed, landed,
                        ss.at[a, side, step - 1], rs.at[a, side, step - 1, c], "tp",
                        jnp.where(me == 0, 1, me - 1),
                    ).wait_recv()

                if step < n - 1:
                    @pl.when(sends(side, step + 1))
                    def _():
                        hop(a, side, step + 1, part(c)).start()

    def square(a, which, index):
        wide = full[a, at_rows(index), :].astype(f32)
        inverse = lax.rsqrt(jnp.mean(wide * wide, axis=-1, keepdims=True) + epsilon)
        inv[which, at_rows(index), :] = jnp.broadcast_to(inverse, (rows, HEAD))

    def squares(a, which, step):
        for side in range(2):
            @pl.when(gets(side, step))
            def _():
                square(a, which, me - step if side == 0 else me + step)

    def multiply(a, right, out, which, c=None, kept=0):
        tile = min(256, right.shape[1])
        features = slice(None) if c is None else part(c)

        @pl.loop(0, right.shape[1] // tile)
        def _(t):
            columns = pl.ds(pl.multiple_of(t * tile, tile), tile)
            held = pl.ds(pl.multiple_of(kept + t * tile, tile), tile)
            product = jnp.dot(
                full[a, :, features], right[features, columns], preferred_element_type=f32
            )
            if c is not None and c > 0:
                product = product + acc[:, held]
            if c is None or c == gather_parts - 1:
                if which is not None:
                    product = product * inv[which, :, :1]
                out[:, columns] = product.astype(bf16)
            else:
                acc[:, held] = product

    def allowed(which):
        owner = jnp.broadcast_to(docs[which : which + 1, :].astype(f32), (seq, seq))
        i = lax.broadcasted_iota(jnp.int32, (seq, seq), 0)
        j = lax.broadcasted_iota(jnp.int32, (seq, seq), 1)
        return (j <= i) & (owner == owner.T)

    def stack(ref, g):
        first = g * group
        return jnp.concatenate(
            [ref[:, (first + h) * HEAD : (first + h + 1) * HEAD] for h in range(group)], axis=0
        )

    def head(ref, g):
        return ref[:, g * HEAD : (g + 1) * HEAD]

    def probabilities(which, g):
        scores = contract_last(stack(q, g), head(k, g)) * scale
        pairs = allowed(which)
        scores = jnp.where(jnp.concatenate([pairs] * group, axis=0), scores, -jnp.inf)
        weights = jnp.exp(scores - jnp.max(scores, axis=-1, keepdims=True))
        return (weights / jnp.sum(weights, axis=-1, keepdims=True)).astype(bf16)

    def attend_back(g):
        weights = probs[g]
        wide = weights.astype(f32)
        stacked = stack(dm, g)
        dprobs = contract_last(stacked, head(v, g))
        inner = jnp.sum(wide * dprobs, axis=-1, keepdims=True)
        dscores = (wide * (dprobs - inner) * scale).astype(bf16)
        dqueries = jnp.dot(dscores, head(k, g), preferred_element_type=f32)
        inverse = inv[0, :, :]
        for h in range(group):
            columns = slice((g * group + h) * HEAD, (g * group + h + 1) * HEAD)
            one = dqueries[h * seq : (h + 1) * seq]
            dq[:, columns] = one.astype(bf16)
            aq[mine, :, columns] = (one * inverse).astype(bf16)
        columns = slice(g * HEAD, (g + 1) * HEAD)
        dkeys = contract_first(dscores, stack(q, g))
        dk[:, columns] = dkeys.astype(bf16)
        ak[mine, :, columns] = (dkeys * inverse).astype(bf16)
        dvalues = contract_first(weights, stacked)
        dv[:, columns] = dvalues.astype(bf16)
        av[mine, :, columns] = (dvalues * inverse).astype(bf16)

    def copy(a, side, dest, c, first, columns):
        toward = 1 - 2 * side
        place = dest - 1 + side
        target = slots.at[a, side, place, :, columns]
        source = sums.at[a, at_rows(dest), columns] if first else target
        return remote(
            source, target, ts.at[a, side, place], tr[a].at[side, place, c], "tp", me + toward
        )

    def landed(a, side, dest, c):
        place = dest - 1 + side
        slot = slots.at[a, side, place, :, cut(a, c)]
        remote(
            slot, slot, ts.at[a, side, place], tr[a].at[side, place, c], "tp",
            jnp.where(me == 0, 1, me - 1),
        ).wait_recv()

    def roles(side, dest):
        if side == 0:
            return me == 0, (me > 0) & (me < dest)
        return me == n - 1, (me < n - 1) & (me > dest)

    def route(side, turn):
        return n - 1 - turn if side == 0 else turn

    def first_send(a, turn, c):
        for side in range(2):
            dest = route(side, turn)

            @pl.when(roles(side, dest)[0])
            def _():
                copy(a, side, dest, c, True, cut(a, c)).start()

    near = jnp.where(2 * me < n, 0, 1)

    def pass_on(a, turn, side, parts=None):
        dest = jnp.where(side == 0, n - 1 - turn, turn)
        place = dest - 1 + side
        upward = (side == 0) & (me > 0) & (me < dest)
        downward = (side == 1) & (me < n - 1) & (me > dest)

        @pl.when(upward | downward)
        def _():
            for c in range(len(cuts[a])) if parts is None else parts:
                columns = cut(a, c)
                landed(a, side, dest, c)
                slots[a, side, place, :, columns] = (
                    slots[a, side, place, :, columns].astype(f32)
                    + sums[a, at_rows(dest), columns].astype(f32)
                ).astype(bf16)
                copy(a, side, dest, c, False, columns).start()

    def pass_all(a, side, turns=range(n - 1)):
        for turn in turns:
            pass_on(a, turn, side)

    def collect(a, c, base):
        columns = cut(a, c)
        mine_sum = sums[a, at_rows(me), columns].astype(f32)
        if base is not None:
            mine_sum = mine_sum + full[base, at_rows(me), columns].astype(f32)
        total[:, columns] = mine_sum
        for side in range(2):
            @pl.when(me > 0 if side == 0 else me < n - 1)
            def _():
                landed(a, side, me, c)
                total[:, columns] += slots[a, side, me - 1 + side, :, columns].astype(f32)

    def spread(a, pairs, halfway=None):
        count = len(cuts[a])
        for c, size in enumerate(cuts[a]):
            base = sum(cuts[a][:c])
            tile = math.gcd(256, size)

            @pl.loop(0, size // tile)
            def _(t):
                features = pl.ds(pl.multiple_of(base + t * tile, tile), tile)
                acc = None
                for left, right in pairs:
                    term = contract_last(left[...], right[features, :])
                    acc = term if acc is None else acc + term
                sums[a, :, features] = acc.astype(bf16)

            first_send(a, 0, c)
            if halfway is not None and c == (count - 1) // 2:
                halfway()
        for turn in range(1, n - 1):
            for c in range(count):
                first_send(a, turn, c)

    loads[0].wait()
    start(0)
    square(0, 0, me)
    loads[1].wait()
    loads[2].wait()
    square(2, 1, me)
    for step in range(1, n):
        arrive(0, step)
        squares(0, 0, step)
        if step == max(n - 2, 1):
            start(1)
    trades = []

    def trade(i, source, target):
        for offset in range(1, copies):
            other = lax.rem(mine + offset, copies)
            one = remote(
                source(other), target, dss.at[offset, i], drs.at[offset, i], "dp", other
            )
            one.start()
            trades.append(one)

    trade(
        0, lambda other: full.at[0, :, pl.ds(pl.multiple_of(other * piece, piece), piece)],
        ncols.at[mine],
    )
    ncols[mine] = full[0, :, pl.ds(pl.multiple_of(mine * piece, piece), piece)]
    for load in loads[3:]:
        load.wait()
    multiply(0, vq, q, 0)
    arrive(1, 1)
    multiply(0, vk, k, 0)
    multiply(0, vv, v, 0)
    for g in range(kv_local):
        probs[g] = probabilities(1, g)
    for step in range(2, n - 1):
        arrive(1, step)
    start(2)
    for c in range(gather_parts):
        if n > 2:
            arrive(1, n - 1, (c,))
        multiply(1, vo, dm, None, c)
    for g in range(kv_local):
        attend_back(g)
    for i, target in enumerate((aq, ak, av)):
        trade(i + 1, lambda other: target.at[mine], target.at[mine])
    spread(0, ((dq, vq), (dk, vk), (dv, vv)))

    for step in range(1, n - 1):
        arrive(2, step)
        squares(2, 1, step)
    for c in range(gather_parts):
        arrive(2, n - 1, (c,))
        if c == gather_parts - 1:
            squares(2, 1, n - 1)
        kept = 0
        for right, out in ((vq, q), (vk, k), (vv, v)):
            multiply(2, right, out, 1, c, kept)
            kept += right.shape[1]
    pass_all(0, near, range(1))
    for g in range(kv_local):
        heads = jnp.dot(
            probabilities(0, g), head(v, g), preferred_element_type=f32
        ).astype(bf16)
        for h in range(group):
            columns = slice((g * group + h) * HEAD, (g * group + h + 1) * HEAD)
            mixed[:, columns] = heads[h * seq : (h + 1) * seq]
    spread(1, ((mixed, vo),), lambda: pass_all(0, near, range(1, n - 1)))
    pass_all(0, 1 - near)

    for one in trades:
        one.wait()
    tile = min(256, piece)

    @pl.loop(0, piece // tile)
    def _(t):
        features = pl.ds(pl.multiple_of(t * tile, tile), tile)
        left = ncols[:, :, features].reshape(copies * seq, tile)
        for right, out in ((aq, wgq), (ak, wgk), (av, wgv)):
            out[features, :] = contract_first(
                left, right[...].reshape(copies * seq, right.shape[2])
            )

    for c in range(len(cuts[0])):
        collect(0, c, None)
    inverse = inv[0, at_rows(me), :1]
    scaled = full[0, at_rows(me), :].astype(f32) * inverse
    centred = total[...] - scaled * jnp.mean(total[...] * scaled, axis=-1, keepdims=True)
    outgoing[0] = (full[1, at_rows(me), :].astype(f32) + inverse * centred).astype(bf16)

    def handoff(a, target, device, columns):
        return remote(
            outgoing.at[a, :, columns], target.at[:, columns], hs.at[a], hr.at[a], "pp", device
        )

    handoff(0, grad_out, behind, every).start()

    pass_on(1, 0, near)
    for turn in range(1, n):
        for c in range(len(cuts[1])):
            pass_on(1, turn - 1, 1 - near, (c,))
            if turn < n - 1:
                pass_on(1, turn, near, (c,))
    for c in range(len(cuts[1])):
        columns = cut(1, c)
        collect(1, c, 2)
        outgoing[1, :, columns] = total[:, columns].astype(bf16)
        handoff(1, act_out, ahead, columns).start()

    for a in range(3):
        for step in range(1, n):
            for side in range(2):
                @pl.when(sends(side, step))
                def _():
                    hop(a, side, step, every).wait_send()
    for a in range(2):
        for turn in range(n - 1):
            for side in range(2):
                dest = route(side, turn)
                first, middle = roles(side, dest)

                @pl.when(first | middle)
                def _():
                    copy(a, side, dest, 0, False, every).wait_send()
    handoff(0, grad_out, behind, every).wait()
    handoff(1, act_out, ahead, every).wait()


def pin(x):
    return pltpu.with_memory_space_constraint(x, pltpu.HBM)


def section_call(n, copies, stages, stash, grad, act, docs, wq, wk, wv, wo):
    rows, width = act.shape
    seq = rows * n
    gather_parts, cuts = chunking(rows, width)
    vmem = pl.BlockSpec(memory_space=pltpu.VMEM)
    hbm = pl.BlockSpec(memory_space=pltpu.HBM)
    heads = wk.shape[1] // HEAD
    group = wq.shape[1] // wk.shape[1]
    piece = width // copies
    outs = [jax.ShapeDtypeStruct((rows, width), bf16)] * 2
    outs += [jax.ShapeDtypeStruct((piece, w.shape[1]), f32) for w in (wq, wk, wv)]
    held = wq.shape[1] + wk.shape[1] + wv.shape[1]
    sem = pltpu.SemaphoreType.DMA
    flops = 2 * seq * width * (3 * wq.shape[1] + 3 * wk.shape[1] + 3 * wv.shape[1] + wo.shape[1])
    return pl.pallas_call(
        functools.partial(section_kernel, n, copies, stages, gather_parts, cuts),
        out_shape=outs,
        in_specs=[hbm] * 8,
        out_specs=[vmem] * len(outs),
        scratch_shapes=[
            pltpu.VMEM(docs.shape, docs.dtype),
            pltpu.VMEM((3, seq, width), bf16),
            pltpu.VMEM((2, seq, HEAD), f32),
        ]
        + [pltpu.VMEM(w.shape, bf16) for w in (wq, wk, wv, wo)]
        + [pltpu.VMEM((seq, w.shape[1]), bf16) for w in (wq, wk, wv, wo, wo)]
        + [pltpu.VMEM((heads, group * seq, seq), bf16)]
        + [pltpu.VMEM((seq, w.shape[1]), bf16) for w in (wq, wk, wv)]
        + [pltpu.VMEM((copies, seq, piece), bf16)]
        + [pltpu.VMEM((copies, seq, w.shape[1]), bf16) for w in (wq, wk, wv)]
        + [
            pltpu.VMEM((seq, held), f32),
            pltpu.VMEM((2, seq, width), bf16),
            pltpu.VMEM((2, 2, n - 1, rows, width), bf16),
            pltpu.VMEM((rows, width), f32),
            pltpu.VMEM((2, rows, width), bf16),
            sem((8,)),
            sem((3, 2, n - 1)), sem((3, 2, n - 1, gather_parts)),
            sem((2, 2, n - 1)),
            *(sem((2, n - 1, len(sizes))) for sizes in cuts),
            sem((copies, 4)), sem((copies, 4)),
            sem((2,)), sem((2,)),
        ],
        compiler_params=pltpu.CompilerParams(
            collective_id=0, has_side_effects=True, vmem_limit_bytes=VMEM_LIMIT
        ),
        cost_estimate=pl.CostEstimate(
            flops=flops, bytes_accessed=30_000_000, transcendentals=0
        ),
    )(*(pin(x) for x in (stash, grad, act, docs, wq, wk, wv, wo)))


def store_kernel(*refs):
    count = (len(refs) - 1) // 2
    sems = refs[-1]
    copies = []
    for i, (source, target) in enumerate(zip(refs[:count], refs[count:-1])):
        pieces = max(1, source.shape[0] // 512)
        size = source.shape[0] // pieces
        for p in range(pieces):
            where = pl.ds(p * size, size)
            one = pltpu.make_async_copy(source.at[where], target.at[where], sems.at[i, p])
            one.start()
            copies.append(one)
    for one in copies:
        one.wait()


def store_call(*arrays):
    pieces = max(1, max(a.shape[0] for a in arrays) // 512)
    return pl.pallas_call(
        store_kernel,
        out_shape=[jax.ShapeDtypeStruct(a.shape, a.dtype) for a in arrays],
        in_specs=[pl.BlockSpec(memory_space=pltpu.VMEM)] * len(arrays),
        out_specs=[pl.BlockSpec(memory_space=pltpu.HBM)] * len(arrays),
        scratch_shapes=[pltpu.SemaphoreType.DMA((len(arrays), pieces))],
        compiler_params=pltpu.CompilerParams(vmem_limit_bytes=20 * 1024 * 1024),
        cost_estimate=pl.CostEstimate(
            flops=10_000_000, bytes_accessed=sum(2 * a.size * a.dtype.itemsize for a in arrays),
            transcendentals=0,
        ),
    )(*arrays)


def body(act_in, stash_in, grad_in, doc_ids, query_weight, key_weight, value_weight, out_weight):
    n, copies, stages = (lax.axis_size(axis) for axis in ("tp", "dp", "pp"))
    made = section_call(
        n, copies, stages, stash_in[0, 0], grad_in[0, 0], act_in[0, 0], doc_ids[0, 0],
        query_weight[0], key_weight[0], value_weight[0], out_weight[0],
    )
    act_out, grad_out, grad_query, grad_key, grad_value = store_call(*made)
    return (
        act_out[None, None], grad_out[None, None],
        grad_query[None], grad_key[None], grad_value[None],
    )


def solution(mesh):
    placed = (
        P("pp", "dp", "tp", None),
        P("pp", "dp", "tp", None),
        P("pp", "dp", "tp", None),
        P("pp", "dp", None, None),
        P("pp", None, "tp"),
        P("pp", None, "tp"),
        P("pp", None, "tp"),
        P("pp", None, "tp"),
    )
    return jax.shard_map(
        body,
        mesh=mesh,
        in_specs=placed,
        out_specs=(
            P("pp", "dp", "tp", None),
            P("pp", "dp", "tp", None),
            P("pp", "dp", "tp"),
            P("pp", "dp", "tp"),
            P("pp", "dp", "tp"),
        ),
        check_vma=False,
    )
```

```python
import functools
import math

import jax
import jax.numpy as jnp
from jax import lax
from jax.experimental import pallas as pl
from jax.experimental.pallas import tpu as pltpu
from jax.sharding import PartitionSpec as P

HEAD = 128
epsilon = 1e-05
MESH = pl.DeviceIdType.MESH
VMEM_LIMIT = 40 * 1024 * 1024
bf16 = jnp.bfloat16
f32 = jnp.float32


def remote(source, target, send_sem, recv_sem, axis, device):
    return pltpu.make_async_remote_copy(
        src_ref=source,
        dst_ref=target,
        send_sem=send_sem,
        recv_sem=recv_sem,
        device_id={axis: device},
        device_id_type=MESH,
    )


def contract_last(left, right):
    return lax.dot_general(left, right, (((1,), (1,)), ((), ())), preferred_element_type=f32)


def contract_first(left, right):
    return lax.dot_general(left, right, (((0,), (0,)), ((), ())), preferred_element_type=f32)


def chunking(rows, width):
    if rows * width < 32 * 4096:
        return (width,), ((width,), (width,))
    eighth = width // 8
    sizes = ((3, 2, 2, 1), (1, 2, 2, 3), (2, 2, 2, 1, 1))
    gathered, *summed = (tuple(eighth * k for k in one) for one in sizes)
    return gathered, tuple(summed)


def section_kernel(
    n, copies, stages, blocks, cuts,
    stash, grad, act, numbers, wq, wk, wv, wo,
    act_out, grad_out, wgq, wgk, wgv,
    docs, full, inv, vq, vk, vv, vo, q, k, v, dm, mixed, probs, dq, dk, dv,
    ncols, aq, ak, av, acc, sums, slots, total, outgoing,
    wsem, ss, rs, ts, tr_back, tr_ahead, dss, drs, hs, hr,
):
    me = lax.axis_index("tp")
    mine = lax.axis_index("dp")
    stage = lax.axis_index("pp")
    rows, width = act.shape
    seq = rows * n
    piece = width // copies
    kv_local = vk.shape[1] // HEAD
    group = vq.shape[1] // (kv_local * HEAD)
    scale = 1.0 / math.sqrt(HEAD)

    def at_rows(index):
        return pl.ds(pl.multiple_of(index * rows, rows), rows)

    loads = []
    pairs = [(own, full.at[a, at_rows(me), :]) for a, own in enumerate((stash, grad, act))]
    pairs += [(wq, vq), (wk, vk), (wv, vv), (wo, vo), (numbers, docs)]
    for i, (hbm, vmem) in enumerate(pairs):
        load = pltpu.make_async_copy(hbm, vmem, wsem.at[i])
        load.start()
        loads.append(load)

    barrier = pltpu.get_barrier_semaphore()

    @pl.when(me > 0)
    def _():
        pl.semaphore_signal(barrier, inc=1, device_id={"tp": me - 1}, device_id_type=MESH)

    @pl.when(me < n - 1)
    def _():
        pl.semaphore_signal(barrier, inc=1, device_id={"tp": me + 1}, device_id_type=MESH)

    for offset in range(1, copies):
        other = lax.rem(mine + offset, copies)
        pl.semaphore_signal(barrier, inc=1, device_id={"dp": other}, device_id_type=MESH)
    ahead, behind = lax.rem(stage + 1, stages), lax.rem(stage + stages - 1, stages)
    for other in (ahead, behind):
        pl.semaphore_signal(barrier, inc=1, device_id={"pp": other}, device_id_type=MESH)
    ends = jnp.where(me > 0, 1, 0) + jnp.where(me < n - 1, 1, 0)
    pl.semaphore_wait(barrier, ends + copies - 1 + 2)

    gather_parts = len(blocks)

    def part(c):
        return pl.ds(sum(blocks[:c]), blocks[c])

    def cut(a, c):
        return pl.ds(sum(cuts[a][:c]), cuts[a][c])

    every = pl.ds(0, width)
    tr = (tr_back, tr_ahead)

    def hop(a, side, step, c, columns):
        toward = 1 if side == 0 else -1
        carried = me - toward * (step - 1)
        block = full.at[a, at_rows(carried), columns]
        return remote(
            block, block, ss.at[a, side, step - 1],
            rs.at[a, side, step - 1, c],
            "tp", me + toward,
        )

    def sends(side, step):
        if side == 0:
            return (me < n - 1) & (me - (step - 1) >= 0)
        return (me > 0) & (me + (step - 1) < n)

    def gets(side, step):
        return (me - step >= 0) if side == 0 else (me + step < n)

    def start(a):
        for c in range(gather_parts):
            for side in range(2):
                @pl.when(sends(side, 1))
                def _():
                    hop(a, side, 1, c, part(c)).start()

    def arrive(a, step, parts=None):
        for c in range(gather_parts) if parts is None else parts:
            for side in range(2):
                toward = 1 if side == 0 else -1

                @pl.when(gets(side, step))
                def _():
                    landed = full.at[a, at_rows(me - toward * step), part(c)]
                    remote(
                        landed, landed,
                        ss.at[a, side, step - 1], rs.at[a, side, step - 1, c], "tp",
                        jnp.where(me == 0, 1, me - 1),
                    ).wait_recv()

                if step < n - 1:
                    @pl.when(sends(side, step + 1))
                    def _():
                        hop(a, side, step + 1, c, part(c)).start()

    def square(a, which, index):
        wide = full[a, at_rows(index), :].astype(f32)
        inverse = lax.rsqrt(jnp.mean(wide * wide, axis=-1, keepdims=True) + epsilon)
        inv[which, at_rows(index), :] = jnp.broadcast_to(inverse, (rows, HEAD))

    def squares(a, which, step):
        for side in range(2):
            @pl.when(gets(side, step))
            def _():
                square(a, which, me - step if side == 0 else me + step)

    def multiply(a, right, out, which, c=None, kept=0):
        tile = math.gcd(1024, right.shape[1])
        features = slice(None) if c is None else part(c)

        @pl.loop(0, right.shape[1] // tile)
        def _(t):
            columns = pl.ds(pl.multiple_of(t * tile, tile), tile)
            held = pl.ds(pl.multiple_of(kept + t * tile, tile), tile)
            product = jnp.dot(
                full[a, :, features], right[features, columns], preferred_element_type=f32
            )
            if c is not None and c > 0:
                product = product + acc[:, held]
            if c is None or c == gather_parts - 1:
                if which is not None:
                    product = product * inv[which, :, :1]
                out[:, columns] = product.astype(bf16)
            else:
                acc[:, held] = product

    def allowed(which):
        owner = jnp.broadcast_to(docs[which : which + 1, :].astype(f32), (seq, seq))
        i = lax.broadcasted_iota(jnp.int32, (seq, seq), 0)
        j = lax.broadcasted_iota(jnp.int32, (seq, seq), 1)
        return (j <= i) & (owner == owner.T)

    def stack(ref, g):
        first = g * group
        return jnp.concatenate(
            [ref[:, (first + h) * HEAD : (first + h + 1) * HEAD] for h in range(group)], axis=0
        )

    def head(ref, g):
        return ref[:, g * HEAD : (g + 1) * HEAD]

    def probabilities(which, g):
        scores = contract_last(stack(q, g), head(k, g)) * scale
        pairs = allowed(which)
        scores = jnp.where(jnp.concatenate([pairs] * group, axis=0), scores, -jnp.inf)
        weights = jnp.exp(scores - jnp.max(scores, axis=-1, keepdims=True))
        return (weights / jnp.sum(weights, axis=-1, keepdims=True)).astype(bf16)

    def attend_back(g):
        weights = probs[g]
        wide = weights.astype(f32)
        stacked = stack(dm, g)
        dprobs = contract_last(stacked, head(v, g))
        inner = jnp.sum(wide * dprobs, axis=-1, keepdims=True)
        dscores = (wide * (dprobs - inner) * scale).astype(bf16)
        dqueries = jnp.dot(dscores, head(k, g), preferred_element_type=f32)
        inverse = inv[0, :, :]
        for h in range(group):
            columns = slice((g * group + h) * HEAD, (g * group + h + 1) * HEAD)
            one = dqueries[h * seq : (h + 1) * seq]
            dq[:, columns] = one.astype(bf16)
            aq[mine, :, columns] = (one * inverse).astype(bf16)
        columns = slice(g * HEAD, (g + 1) * HEAD)
        dkeys = contract_first(dscores, stack(q, g))
        dk[:, columns] = dkeys.astype(bf16)
        ak[mine, :, columns] = (dkeys * inverse).astype(bf16)
        dvalues = contract_first(weights, stacked)
        dv[:, columns] = dvalues.astype(bf16)
        av[mine, :, columns] = (dvalues * inverse).astype(bf16)

    def copy(a, side, dest, c, first, columns):
        toward = 1 - 2 * side
        place = dest - 1 + side
        target = slots.at[a, side, place, :, columns]
        source = sums.at[a, at_rows(dest), columns] if first else target
        return remote(
            source, target, ts.at[a, side, place], tr[a].at[side, place, c], "tp", me + toward
        )

    def landed(a, side, dest, c):
        place = dest - 1 + side
        slot = slots.at[a, side, place, :, cut(a, c)]
        remote(
            slot, slot, ts.at[a, side, place], tr[a].at[side, place, c], "tp",
            jnp.where(me == 0, 1, me - 1),
        ).wait_recv()

    def roles(side, dest):
        if side == 0:
            return me == 0, (me > 0) & (me < dest)
        return me == n - 1, (me < n - 1) & (me > dest)

    def route(side, turn):
        return n - 1 - turn if side == 0 else turn

    def first_send(a, turn, c):
        for side in range(2):
            dest = route(side, turn)

            @pl.when(roles(side, dest)[0])
            def _():
                copy(a, side, dest, c, True, cut(a, c)).start()

    near = jnp.where(2 * me < n, 0, 1)

    def pass_on(a, turn, side, parts=None):
        dest = jnp.where(side == 0, n - 1 - turn, turn)
        place = dest - 1 + side
        upward = (side == 0) & (me > 0) & (me < dest)
        downward = (side == 1) & (me < n - 1) & (me > dest)

        @pl.when(upward | downward)
        def _():
            for c in range(len(cuts[a])) if parts is None else parts:
                columns = cut(a, c)
                landed(a, side, dest, c)
                slots[a, side, place, :, columns] = (
                    slots[a, side, place, :, columns].astype(f32)
                    + sums[a, at_rows(dest), columns].astype(f32)
                ).astype(bf16)
                copy(a, side, dest, c, False, columns).start()

    def pass_all(a, side, turns=range(n - 1)):
        for turn in turns:
            pass_on(a, turn, side)

    def collect(a, c, base):
        columns = cut(a, c)
        mine_sum = sums[a, at_rows(me), columns].astype(f32)
        if base is not None:
            mine_sum = mine_sum + full[base, at_rows(me), columns].astype(f32)
        total[:, columns] = mine_sum
        for side in range(2):
            @pl.when(me > 0 if side == 0 else me < n - 1)
            def _():
                landed(a, side, me, c)
                total[:, columns] += slots[a, side, me - 1 + side, :, columns].astype(f32)

    def spread(a, pairs, halfway=None):
        count = len(cuts[a])
        early = 2 if a == 0 and n > 2 and count > 2 else 0
        for c, size in enumerate(cuts[a]):
            base = sum(cuts[a][:c])
            tile = math.gcd(512, size)

            @pl.loop(0, size // tile)
            def _(t):
                features = pl.ds(pl.multiple_of(base + t * tile, tile), tile)
                acc = None
                for left, right in pairs:
                    term = contract_last(left[...], right[features, :])
                    acc = term if acc is None else acc + term
                sums[a, :, features] = acc.astype(bf16)

            first_send(a, 0, c)
            if c < early:
                first_send(a, 1, c)
            if halfway is not None and c == (count - 1) // 2:
                halfway()
        for turn in range(1, n - 1):
            for c in range(early if turn == 1 else 0, count):
                first_send(a, turn, c)

    def gather_sent():
        for a in range(3):
            for step in range(1, n):
                for side in range(2):
                    @pl.when(sends(side, step))
                    def _():
                        hop(a, side, step, 0, every).wait_send()

    def sums_sent(a):
        for turn in range(n - 1):
            for side in range(2):
                dest = route(side, turn)
                first, middle = roles(side, dest)

                @pl.when(first | middle)
                def _():
                    copy(a, side, dest, 0, False, every).wait_send()

    loads[0].wait()
    start(0)
    square(0, 0, me)
    loads[1].wait()
    loads[2].wait()
    square(2, 1, me)
    for step in range(1, n):
        arrive(0, step)
        squares(0, 0, step)
        if step == max(n - 2, 1):
            start(1)
    trades = []

    def trade(i, source, target):
        for offset in range(1, copies):
            other = lax.rem(mine + offset, copies)
            one = remote(
                source(other), target, dss.at[offset - 1, i], drs.at[offset - 1, i], "dp", other
            )
            one.start()
            trades.append(one)

    trade(
        0, lambda other: full.at[0, :, pl.ds(pl.multiple_of(other * piece, piece), piece)],
        ncols.at[mine],
    )
    ncols[mine] = full[0, :, pl.ds(pl.multiple_of(mine * piece, piece), piece)]
    for load in loads[3:]:
        load.wait()
    multiply(0, vq, q, 0)
    arrive(1, 1)
    multiply(0, vk, k, 0)
    multiply(0, vv, v, 0)
    for g in range(kv_local):
        probs[g] = probabilities(1, g)
    for step in range(2, n - 1):
        arrive(1, step)
    start(2)
    for c in range(gather_parts):
        if n > 2:
            arrive(1, n - 1, (c,))
        multiply(1, vo, dm, None, c)
    for g in range(kv_local):
        attend_back(g)
    for i, target in enumerate((aq, ak, av)):
        trade(i + 1, lambda other: target.at[mine], target.at[mine])
    spread(0, ((dq, vq), (dk, vk), (dv, vv)))

    for step in range(1, n - 1):
        arrive(2, step)
        squares(2, 1, step)
    for c in range(gather_parts):
        arrive(2, n - 1, (c,))
        if c == gather_parts - 1:
            squares(2, 1, n - 1)
        kept = 0
        for right, out in ((vq, q), (vk, k), (vv, v)):
            multiply(2, right, out, 1, c, kept)
            kept += right.shape[1]
    pass_all(0, near, range(1))
    for g in range(kv_local):
        heads = jnp.dot(
            probabilities(0, g), head(v, g), preferred_element_type=f32
        ).astype(bf16)
        for h in range(group):
            columns = slice((g * group + h) * HEAD, (g * group + h + 1) * HEAD)
            mixed[:, columns] = heads[h * seq : (h + 1) * seq]
    spread(1, ((mixed, vo),), lambda: pass_all(0, near, range(1, n - 1)))
    pass_all(0, 1 - near)

    for one in trades:
        one.wait()
    tile = min(256, piece)

    @pl.loop(0, piece // tile)
    def _(t):
        features = pl.ds(pl.multiple_of(t * tile, tile), tile)
        left = ncols[:, :, features].reshape(copies * seq, tile)
        for right, out in ((aq, wgq), (ak, wgk), (av, wgv)):
            out[features, :] = contract_first(
                left, right[...].reshape(copies * seq, right.shape[2])
            )

    for c in range(len(cuts[0])):
        collect(0, c, None)
    inverse = inv[0, at_rows(me), :1]
    scaled = full[0, at_rows(me), :].astype(f32) * inverse
    centred = total[...] - scaled * jnp.mean(total[...] * scaled, axis=-1, keepdims=True)
    outgoing[0] = (full[1, at_rows(me), :].astype(f32) + inverse * centred).astype(bf16)

    def handoff(a, target, device, columns):
        return remote(
            outgoing.at[a, :, columns], target.at[:, columns], hs.at[a], hr.at[a], "pp", device
        )

    handoff(0, grad_out, behind, every).start()

    gather_sent()
    pass_on(1, 0, near)
    for turn in range(1, n):
        for c in range(len(cuts[1])):
            pass_on(1, turn - 1, 1 - near, (c,))
            if turn < n - 1:
                pass_on(1, turn, near, (c,))
    sums_sent(0)
    handoff(0, grad_out, behind, every).wait()
    for c in range(len(cuts[1])):
        columns = cut(1, c)
        collect(1, c, 2)
        outgoing[1, :, columns] = total[:, columns].astype(bf16)
        handoff(1, act_out, ahead, columns).start()

    sums_sent(1)
    handoff(1, act_out, ahead, every).wait()


def pin(x):
    return pltpu.with_memory_space_constraint(x, pltpu.HBM)


def section_call(n, copies, stages, stash, grad, act, docs, wq, wk, wv, wo):
    rows, width = act.shape
    seq = rows * n
    blocks, cuts = chunking(rows, width)
    vmem = pl.BlockSpec(memory_space=pltpu.VMEM)
    hbm = pl.BlockSpec(memory_space=pltpu.HBM)
    heads = wk.shape[1] // HEAD
    group = wq.shape[1] // wk.shape[1]
    piece = width // copies
    outs = [jax.ShapeDtypeStruct((rows, width), bf16)] * 2
    outs += [jax.ShapeDtypeStruct((piece, w.shape[1]), f32) for w in (wq, wk, wv)]
    held = wq.shape[1] + wk.shape[1] + wv.shape[1]
    sem = pltpu.SemaphoreType.DMA
    flops = 2 * seq * width * (3 * wq.shape[1] + 3 * wk.shape[1] + 3 * wv.shape[1] + wo.shape[1])
    return pl.pallas_call(
        functools.partial(section_kernel, n, copies, stages, blocks, cuts),
        out_shape=outs,
        in_specs=[hbm] * 8,
        out_specs=[vmem] * len(outs),
        scratch_shapes=[
            pltpu.VMEM(docs.shape, docs.dtype),
            pltpu.VMEM((3, seq, width), bf16),
            pltpu.VMEM((2, seq, HEAD), f32),
        ]
        + [pltpu.VMEM(w.shape, bf16) for w in (wq, wk, wv, wo)]
        + [pltpu.VMEM((seq, w.shape[1]), bf16) for w in (wq, wk, wv, wo, wo)]
        + [pltpu.VMEM((heads, group * seq, seq), bf16)]
        + [pltpu.VMEM((seq, w.shape[1]), bf16) for w in (wq, wk, wv)]
        + [pltpu.VMEM((copies, seq, piece), bf16)]
        + [pltpu.VMEM((copies, seq, w.shape[1]), bf16) for w in (wq, wk, wv)]
        + [
            pltpu.VMEM((seq, held), f32),
            pltpu.VMEM((2, seq, width), bf16),
            pltpu.VMEM((2, 2, n - 1, rows, width), bf16),
            pltpu.VMEM((rows, width), f32),
            pltpu.VMEM((2, rows, width), bf16),
            sem((8,)),
            sem((3, 2, n - 1)), sem((3, 2, n - 1, len(blocks))),
            sem((2, 2, n - 1)),
            *(sem((2, n - 1, len(sizes))) for sizes in cuts),
            sem((copies - 1, 4)), sem((copies - 1, 4)),
            sem((2,)), sem((2,)),
        ],
        compiler_params=pltpu.CompilerParams(
            collective_id=0, has_side_effects=True, vmem_limit_bytes=VMEM_LIMIT
        ),
        cost_estimate=pl.CostEstimate(
            flops=flops, bytes_accessed=30_000_000, transcendentals=0
        ),
    )(*(pin(x) for x in (stash, grad, act, docs, wq, wk, wv, wo)))


def store_pieces(array):
    return max(1, array.size * array.dtype.itemsize // 2**21)


def store_kernel(*refs):
    count = (len(refs) - 1) // 2
    sems = refs[-1]
    copies = []
    used = 0
    for source, target in zip(refs[:count], refs[count:-1]):
        pieces = store_pieces(source)
        size = source.shape[0] // pieces
        for p in range(pieces):
            where = pl.ds(p * size, size)
            one = pltpu.make_async_copy(source.at[where], target.at[where], sems.at[used])
            used += 1
            one.start()
            copies.append(one)
    for one in copies:
        one.wait()


def store_call(*arrays):
    pieces = sum(store_pieces(a) for a in arrays)
    return pl.pallas_call(
        store_kernel,
        out_shape=[jax.ShapeDtypeStruct(a.shape, a.dtype) for a in arrays],
        in_specs=[pl.BlockSpec(memory_space=pltpu.VMEM)] * len(arrays),
        out_specs=[pl.BlockSpec(memory_space=pltpu.HBM)] * len(arrays),
        scratch_shapes=[pltpu.SemaphoreType.DMA((pieces,))],
        compiler_params=pltpu.CompilerParams(vmem_limit_bytes=20 * 1024 * 1024),
        cost_estimate=pl.CostEstimate(
            flops=10_000_000, bytes_accessed=sum(2 * a.size * a.dtype.itemsize for a in arrays),
            transcendentals=0,
        ),
    )(*arrays)


def body(act_in, stash_in, grad_in, doc_ids, query_weight, key_weight, value_weight, out_weight):
    n, copies, stages = (lax.axis_size(axis) for axis in ("tp", "dp", "pp"))
    made = section_call(
        n, copies, stages, stash_in[0, 0], grad_in[0, 0], act_in[0, 0], doc_ids[0, 0],
        query_weight[0], key_weight[0], value_weight[0], out_weight[0],
    )
    act_out, grad_out, grad_query, grad_key, grad_value = store_call(*made)
    return (
        act_out[None, None], grad_out[None, None],
        grad_query[None], grad_key[None], grad_value[None],
    )


def solution(mesh):
    placed = (
        P("pp", "dp", "tp", None),
        P("pp", "dp", "tp", None),
        P("pp", "dp", "tp", None),
        P("pp", "dp", None, None),
        P("pp", None, "tp"),
        P("pp", None, "tp"),
        P("pp", None, "tp"),
        P("pp", None, "tp"),
    )
    return jax.shard_map(
        body,
        mesh=mesh,
        in_specs=placed,
        out_specs=(
            P("pp", "dp", "tp", None),
            P("pp", "dp", "tp", None),
            P("pp", "dp", "tp"),
            P("pp", "dp", "tp"),
            P("pp", "dp", "tp"),
        ),
        check_vma=False,
    )
```
